32 devices in a mesh: row: 8 (over z, y), col: 4 (over x, core).
Axes of the slice: x: 2, y: 2, z: 4, core: 2. Of those that a mesh axis runs over, the one named last changes fastest.
Arguments:
- field: float32 [512, 64, 8, 512], P('row', 'col'), may hold values from -6 to 6
- modes: int32 [3, 256], replicated, may hold values from 0 to 511, as said below
Outputs:
- spectrum: float32 [64, 512, 8, 512], P(None, 'col', None, 'row')
- localized: float32 [512, 512], replicated
The draws below stay inside these ranges and needn't reach their ends.
Inputs may be any that keep to these rules, and one draw needn't show every extreme that they name: `modes`: row 0 holds kx in 0 to 255, row 1 ky in 0 to 511, row 2 kz in 0 to 63; triples may repeat.
All inputs are finite; a program needn't handle non-finite values.
Results may differ from the reference program's by a relative error of at most 0.00013.
Values sent between devices are 32-bit elements; how exact they have to be, the bound alone decides.
A program may use at most 192 MiB of HBM per device.

```python
import math
import jax
import jax.numpy as jnp
from jax import lax

NX = 512
NY = 512
NZ = 64
MEMBERS = 8
MODES = 256
REACH = 64


def draw_modes(key, part):
    first_key, second_key, third_key = jax.random.split(jax.random.fold_in(key, 7), 3)
    first = jax.random.randint(first_key, (MODES,), 0, NX // 2)
    second = jax.random.randint(second_key, (MODES,), 0, NY)
    third = jax.random.randint(third_key, (MODES,), 0, NZ)
    return jnp.stack([first, second, third]).astype(jnp.int32)


def steps_of(rng, shape, pieces, least, largest):
    loudness = 1.0
    for dim, parts in pieces:
        heights = jax.random.uniform(jax.random.fold_in(jax.random.fold_in(rng, 6), dim), (parts,), jnp.float32, least / len(pieces), largest / len(pieces))
        loudness = loudness * jnp.repeat(jnp.exp(heights), shape[dim] // parts).reshape((-1,) + (1,) * (len(shape) - 1 - dim))
    return loudness


def bell_draw(rng, extent, scale, reach, cuts=(), kind=jnp.bfloat16):
    entries = jax.random.normal(rng, extent, jnp.float32) * scale
    if len(cuts) > 0:
        entries = steps_of(rng, extent, cuts, -0.22, 0.18) * entries
    return jnp.clip(entries, min=-reach, max=reach).astype(kind)


def setup_inputs(seed: int = 0) -> dict:
    streams_of = jax.random.split(jax.random.key(seed), 3)
    return {
        "field": bell_draw(streams_of[0], (NY, NZ, MEMBERS, NX), 1.0, 6.0, ((0, 8), (1, 4)), jnp.float32),
        "modes": draw_modes(jax.random.fold_in(streams_of[2], 71), 0),
    }


def taper_of(modes):
    first = modes[0].astype(jnp.float32)
    second = jnp.where(modes[1] < NY // 2, modes[1], modes[1] - NY).astype(jnp.float32)
    third = jnp.where(modes[2] < NZ // 2, modes[2], modes[2] - NZ).astype(jnp.float32)
    first = jnp.concatenate([first, first])
    second = jnp.concatenate([second, second])
    third = jnp.concatenate([third, third])
    dist = (first[:, None] - first[None, :]) ** 2 + (second[:, None] - second[None, :]) ** 2
    dist = dist + (third[:, None] - third[None, :]) ** 2
    return jnp.exp(-dist / (2.0 * REACH * REACH))

def covariance_of(coef, modes):
    anomaly = coef - lax.optimization_barrier(jnp.mean(coef, axis=0, keepdims=True))
    cov = jnp.dot(anomaly.T, anomaly, precision=lax.Precision.HIGHEST) / (MEMBERS - 1)
    return cov * taper_of(modes)

def reference(field, modes):
    factor = 1.0 / math.sqrt(NX * NY * NZ)

    def one_member(member):
        whole = jnp.fft.fftn(member)[:, :, :NX // 2] * factor
        whole = jnp.transpose(whole, (1, 0, 2))
        paired = jnp.stack([jnp.real(whole), jnp.imag(whole)], axis=-1)
        return paired.reshape(NZ, NY, NX).astype(jnp.float32)
    stacked = lax.map(one_member, jnp.transpose(field, (2, 0, 1, 3)))
    spectrum = jnp.transpose(stacked, (1, 2, 0, 3))
    real_rows = spectrum[modes[2], modes[1], :, 2 * modes[0]]
    imag_rows = spectrum[modes[2], modes[1], :, 2 * modes[0] + 1]
    coef = jnp.concatenate([real_rows.T, imag_rows.T], axis=1)
    return (spectrum, covariance_of(coef, modes))
```

```python
import functools
import math

import jax
import jax.numpy as jnp
import numpy as np
from jax import lax
from jax.experimental import pallas as pl
from jax.experimental.pallas import tpu as pltpu
from jax.experimental.layout import Layout, with_layout_constraint
from jax.sharding import PartitionSpec as P

NX = 512
NY = 512
NZ = 64
REACH = 64


highest = lax.Precision.HIGHEST
high = lax.Precision.HIGH
PIECES = 2


def tables(length, count):
    points = lax.iota(jnp.int32, length)
    waves = lax.iota(jnp.int32, count)
    phase = points[:, None] * waves[None, :] % length
    angle = phase.astype(jnp.float32) * (2.0 * math.pi / length)
    return (jnp.cos(angle), jnp.sin(angle))


def taper_of(modes, size_y, size_z, reach):
    first = modes[0].astype(jnp.float32)
    second = jnp.where(modes[1] < size_y // 2, modes[1], modes[1] - size_y).astype(jnp.float32)
    third = jnp.where(modes[2] < size_z // 2, modes[2], modes[2] - size_z).astype(jnp.float32)
    first = jnp.concatenate([first, first])
    second = jnp.concatenate([second, second])
    third = jnp.concatenate([third, third])
    dist = (first[:, None] - first[None, :]) ** 2 + (second[:, None] - second[None, :]) ** 2
    dist = dist + (third[:, None] - third[None, :]) ** 2
    return jnp.exp(-dist / (2.0 * reach * reach))


def twiddle(length, count, scale):
    cos, sin = tables(length, count)
    cos, sin = cos * scale, sin * scale
    return jnp.stack([jnp.stack([cos, sin]), jnp.stack([-sin, cos])])


MESH = pl.DeviceIdType.MESH
LANES = 128
SUB = 8


def split(value):
    top = value.astype(jnp.bfloat16)
    rest = (value - top.astype(jnp.float32)).astype(jnp.bfloat16)
    return top, rest


def waves_of(length, scale):
    j = np.arange(length)
    coarse = 2.0 * np.pi * (np.arange(0, length, SUB)[:, None] * j[None, :] % length) / length
    fine = 2.0 * np.pi * (np.arange(SUB)[:, None] * j[None, :] % length) / length
    coarse = np.stack([np.cos(coarse), np.sin(coarse)]) * scale
    fine = np.stack([np.cos(fine), np.sin(fine)])
    return coarse.astype(np.float32), fine.astype(np.float32)


def cmul(a, c, s):
    re, im = a
    if c == 1.0 and s == 0.0:
        return a
    if c == 0.0 and s == 1.0:
        return im, -re
    return re * c + im * s, im * c - re * s


def fft(items):
    n = len(items)
    if n == 1:
        return items
    even, odd = fft(items[0::2]), fft(items[1::2])
    out = [None] * n
    for k in range(n // 2):
        er, ei = even[k]
        if 8 * k == n or 8 * k == 3 * n:
            r, i = odd[k]
            h = math.sqrt(0.5)
            if 8 * k == n:
                tr, ti = (r + i) * h, (i - r) * h
            else:
                tr, ti = (i - r) * h, (r + i) * (-h)
        elif k == 0:
            tr, ti = odd[k]
        elif 4 * k == n:
            tr, ti = odd[k][1], None
        else:
            angle = 2.0 * math.pi * k / n
            tr, ti = cmul(odd[k], math.cos(angle), math.sin(angle))
        if ti is None:
            r = odd[k][0]
            out[k] = (er + tr, ei - r)
            out[k + n // 2] = (er - tr, ei + r)
        else:
            out[k] = (er + tr, ei + ti)
            out[k + n // 2] = (er - tr, ei - ti)
    return out


class Plan:
    def __init__(self, shape, rows, cols):
        self.near, self.thick, self.members, self.width = shape
        self.rows, self.cols = rows, cols
        self.length = self.near * rows
        self.depth = self.thick * cols
        self.waves = self.width // 2 // rows
        self.local_y = self.length // cols
        self.parts = self.waves // SUB
        self.pieces = self.members * self.parts
        self.lanes = self.near * self.thick
        self.tiles = self.lanes // LANES
        self.slabs = rows * self.tiles

    def fits(self):
        def power(n):
            return n > 1 and n & (n - 1) == 0

        return (
            power(self.rows)
            and power(self.cols)
            and self.waves % SUB == 0
            and self.near * 2 == LANES
            and self.local_y == LANES
            and self.thick % 4 == 0
            and self.rows % 2 == 0
            and self.slabs == self.cols * self.thick
            and self.depth == 64
            and self.width % 256 == 0
            and self.width == self.length
        )


def kernel(plan, factor, field, coarse, fine, out, A, B, D, xtab, ytab, lines, stage, row_send, row_recv, col_send, col_recv, in_sem, out_sem):
    R, C, H, T = plan.rows, plan.cols, plan.parts, plan.tiles
    near, thick = plan.near, plan.thick
    row, col = lax.axis_index("row"), lax.axis_index("col")

    def row_peer(k):
        return (row ^ k, col)

    def col_peer(k):
        return (row, col ^ k)

    row_order = list(range(R // 2, R)) + list(range(1, R // 2))
    col_order = list(range(C // 2, C)) + list(range(1, C // 2))

    def load(m, slot):
        return [
            pltpu.make_async_copy(field.at[:, z, m, :], lines.at[slot, pl.ds(z * near, near), :], in_sem.at[slot])
            for z in range(thick)
        ]

    for copy in load(0, 0):
        copy.start()

    barrier = pltpu.get_barrier_semaphore()
    for k in range(1, R):
        pl.semaphore_signal(barrier, inc=1, device_id=row_peer(k), device_id_type=MESH)
    for k in range(1, C):
        pl.semaphore_signal(barrier, inc=1, device_id=col_peer(k), device_id_type=MESH)

    fc, fs = fine[0], fine[1]

    def x_rows(i, _):
        h, r = i // R, i % R
        a = r * H + h
        uc, us = coarse[0, pl.ds(a, 1), :], coarse[1, pl.ds(a, 1), :]
        block = jnp.concatenate([uc * fc - us * fs, -(us * fc + uc * fs)], axis=0)
        top, rest = split(block)
        at = pl.ds(pl.multiple_of(i * 2 * SUB, 2 * SUB), 2 * SUB)
        xtab[0, at, :] = top
        xtab[1, at, :] = rest
        return 0

    lax.fori_loop(0, H * R, x_rows, 0)

    pl.semaphore_wait(barrier, R + C - 2)

    def row_copy(p, k):
        return pltpu.make_async_remote_copy(
            A.at[p, pl.ds((row ^ k) * T, T)],
            B.at[p, pl.ds(row * T, T)],
            row_send.at[p],
            row_recv.at[p, k],
            device_id=row_peer(k),
            device_id_type=MESH,
        )

    def row_wait(p, k):
        return pltpu.make_async_remote_copy(
            A.at[p, pl.ds((row ^ k) * T, T)],
            B.at[p, pl.ds((row ^ k) * T, T)],
            row_send.at[p],
            row_recv.at[p, k],
            device_id=row_peer(k),
            device_id_type=MESH,
        )

    def col_copy(p, k):
        return pltpu.make_async_remote_copy(
            A.at[p, pl.ds((col ^ k) * thick, thick)],
            D.at[p, pl.ds(col * thick, thick)],
            col_send.at[p],
            col_recv.at[p, k],
            device_id=col_peer(k),
            device_id_type=MESH,
        )

    def col_wait(p, k):
        return pltpu.make_async_remote_copy(
            A.at[p, pl.ds((col ^ k) * thick, thick)],
            D.at[p, pl.ds((col ^ k) * thick, thick)],
            col_send.at[p],
            col_recv.at[p, k],
            device_id=col_peer(k),
            device_id_type=MESH,
        )

    def contract(a, b):
        return lax.dot_general(a, b, (((1,), (1,)), ((), ())), preferred_element_type=jnp.float32)

    chunk = 2 * LANES

    for m in range(plan.members):
        slot = m % 2
        if m + 1 < plan.members:
            for copy in load(m + 1, 1 - slot):
                copy.start()
        for copy in load(m, slot):
            copy.wait()

        def x_step(g, _):
            at = pl.ds(pl.multiple_of(g * chunk, chunk), chunk)
            top, rest = split(lines[slot, at, :])
            got = contract(xtab[0], top) + (contract(xtab[0], rest) + contract(xtab[1], top))
            for h in range(H):
                for r in range(R):
                    base = (h * R + r) * 2 * SUB
                    for t in range(chunk // LANES):
                        A[m * H + h, r * T + g * (chunk // LANES) + t] = got[base : base + 2 * SUB, t * LANES : (t + 1) * LANES]
            return 0

        lax.fori_loop(0, plan.lanes // chunk, x_step, 0)
        for h in range(H):
            p = m * H + h
            mine = pl.ds(row * T, T)
            B[p, mine] = A[p, mine]
            for k in row_order:
                row_copy(p, k).start()

    length = plan.length

    def y_rows(i, _):
        blocks = []
        for b in range(2):
            a = 2 * i + b
            uc, us = coarse[0, pl.ds(a, 1), :], coarse[1, pl.ds(a, 1), :]
            blocks.append(jnp.concatenate([uc * fc - us * fs, us * fc + uc * fs], axis=1))
        top, rest = split(jnp.concatenate(blocks, axis=0) * factor)
        at = pl.ds(pl.multiple_of(i * 2 * SUB, 2 * SUB), 2 * SUB)
        ytab[0, at, :] = top
        ytab[1, at, :] = rest
        return 0

    lax.fori_loop(0, length // (2 * SUB), y_rows, 0)

    low = lax.broadcasted_iota(jnp.int32, (T * 2 * SUB, LANES), 1) < near

    def y_step(p):
        evens, odds = [], []
        for t in range(R // 2):
            v0 = B[p, 2 * t * T : (2 * t + 1) * T].reshape(T * 2 * SUB, LANES)
            v1 = B[p, (2 * t + 1) * T : (2 * t + 2) * T].reshape(T * 2 * SUB, LANES)
            evens.append(jnp.where(low, v0, pltpu.roll(v1, near, 1)))
            odds.append(jnp.where(low, pltpu.roll(v0, near, 1), v1))
        left = jnp.concatenate([jnp.concatenate(evens, axis=1), jnp.concatenate(odds, axis=1)], axis=0)
        top, rest = split(left)

        def times(a, b):
            return jnp.dot(a, b, preferred_element_type=jnp.float32)

        for c in range(C):
            at_c = slice(c * LANES, (c + 1) * LANES)
            at_s = slice(length + c * LANES, length + (c + 1) * LANES)

            def product(at):
                return times(top, ytab[0, :, at]) + (times(rest, ytab[0, :, at]) + times(top, ytab[1, :, at]))

            both = product(at_c).reshape(thick, 2, SUB, LANES), product(at_s).reshape(thick, 2, SUB, LANES)
            re = both[0][:, 0] + both[1][:, 1]
            im = both[0][:, 1] - both[1][:, 0]
            A[p, c * thick : (c + 1) * thick, 0:SUB] = re
            A[p, c * thick : (c + 1) * thick, SUB : 2 * SUB] = im

    def slab(z):
        inner = z % thick
        return z // thick * thick + inner % 2 * (thick // 2) + inner // 2

    eight = 8

    def out_copy(p, slot):
        m, h = p // H, p % H
        q = pl.ds(pl.multiple_of(h * 2 * SUB, 2 * SUB), 2 * SUB)
        return pltpu.make_async_copy(stage.at[slot], out.at[:, m, q, :], out_sem.at[slot])

    def z_step(p, slot):
        for z0 in range(eight):
            items = []
            for z1 in range(eight):
                s = slab(z1 * eight + z0)
                items.append((D[p, s, 0:SUB], D[p, s, SUB : 2 * SUB]))
            for k0, value in enumerate(fft(items)):
                angle = 2.0 * math.pi * z0 * k0 / 64
                exact = z0 * k0 == 0
                re, im = value if exact else cmul(value, math.cos(angle), math.sin(angle))
                s = slab(k0 * eight + z0)
                D[p, s, 0:SUB] = re
                D[p, s, SUB : 2 * SUB] = im
        for k0 in range(eight):
            items = []
            for z0 in range(eight):
                s = slab(k0 * eight + z0)
                items.append((D[p, s, 0:SUB], D[p, s, SUB : 2 * SUB]))
            for k1, (re, im) in enumerate(fft(items)):
                stage[slot, k0 + eight * k1, pl.ds(0, SUB, stride=2), :] = re
                stage[slot, k0 + eight * k1, pl.ds(1, SUB, stride=2), :] = im

    def finish(p):
        slot = p % 2

        @pl.when(p >= 2)
        def _():
            out_copy(p - 2, slot).wait()

        for k in col_order:
            col_wait(p, k).wait_recv()
        z_step(p, slot)
        out_copy(p, slot).start()

    def step(p, _):
        for k in row_order:
            row_wait(p, k).wait_recv()
        for k in row_order:
            row_wait(p, k).wait_send()
        y_step(p)
        mine = pl.ds(col * thick, thick)
        D[p, mine] = A[p, mine]
        for k in col_order:
            col_copy(p, k).start()

        @pl.when(p >= 1)
        def _():
            finish(p - 1)

        return 0

    lax.fori_loop(0, plan.pieces, step, 0)
    finish(plan.pieces - 1)
    for p in (plan.pieces - 2, plan.pieces - 1):
        out_copy(p, p % 2).wait()

    def drain(p, _):
        for k in col_order:
            col_copy(p, k).wait_send()
        return 0

    lax.fori_loop(0, plan.pieces, drain, 0)


def exchanged(plan, field, factor):
    coarse, fine = waves_of(plan.length, 1.0)
    block = (plan.pieces, plan.slabs, 2 * SUB, LANES)
    return pl.pallas_call(
        functools.partial(kernel, plan, factor),
        out_shape=jax.ShapeDtypeStruct((plan.depth, plan.members, 2 * plan.waves, plan.local_y), jnp.float32),
        in_specs=[
            pl.BlockSpec(memory_space=pl.ANY),
            pl.BlockSpec(memory_space=pltpu.VMEM),
            pl.BlockSpec(memory_space=pltpu.VMEM),
        ],
        out_specs=pl.BlockSpec(memory_space=pl.ANY),
        scratch_shapes=[
            pltpu.VMEM(block, jnp.float32),
            pltpu.VMEM(block, jnp.float32),
            pltpu.VMEM(block, jnp.float32),
            pltpu.VMEM((2, plan.width, plan.width), jnp.bfloat16),
            pltpu.VMEM((2, plan.length, 2 * plan.length), jnp.bfloat16),
            pltpu.VMEM((2, plan.lanes, plan.width), jnp.float32),
            pltpu.VMEM((2, plan.depth, 2 * SUB, LANES), jnp.float32),
            pltpu.SemaphoreType.DMA((plan.pieces,)),
            pltpu.SemaphoreType.DMA((plan.pieces, plan.rows)),
            pltpu.SemaphoreType.DMA((plan.pieces,)),
            pltpu.SemaphoreType.DMA((plan.pieces, plan.cols)),
            pltpu.SemaphoreType.DMA((2,)),
            pltpu.SemaphoreType.DMA((2,)),
        ],
        compiler_params=pltpu.CompilerParams(collective_id=0, has_side_effects=True, vmem_limit_bytes=67043328),
    )(field, jnp.asarray(coarse), jnp.asarray(fine))


def general(field):
    members = field.shape[2]
    width = field.shape[3]
    rows, cols = lax.axis_size("row"), lax.axis_size("col")
    near, thick = field.shape[0], field.shape[1]
    length, depth = near * rows, thick * cols
    waves = width // 2 // rows
    pieces = PIECES if waves % PIECES == 0 else 1
    part = waves // pieces
    local_y = length // cols
    factor = 1.0 / math.sqrt(NX * NY * NZ)
    cos_x, sin_x = tables(width, width // 2)
    x_table = jnp.stack([cos_x, -sin_x]).reshape(2, width, rows, pieces, part)
    y_table = twiddle(length, length, 1.0).reshape(2, 2, rows, near, length)
    z_table = twiddle(depth, depth, factor).reshape(2, 2, cols, thick, depth)
    flat = field.reshape(near, thick * members, width)
    outs = []
    for piece in range(pieces):
        lines = jnp.einsum("cxrk,ylx->rckyl", x_table[:, :, :, piece], flat, precision=high)
        lines = with_layout_constraint(lines, Layout((0, 1, 2, 3, 4)))
        gathered = lax.all_to_all(lines, "row", split_axis=0, concat_axis=0, tiled=True)
        gathered = with_layout_constraint(gathered, Layout((0, 1, 2, 3, 4)))
        gathered = gathered.reshape(rows, 2, part, near, thick, members)
        ytrans = jnp.einsum("dcsyf,sckyzm->dkmzf", y_table, gathered, precision=high)
        ytrans = ytrans.reshape(2, part, members, thick, cols, local_y)
        ytrans = jnp.transpose(ytrans, (4, 0, 1, 2, 3, 5))
        levels = lax.all_to_all(ytrans, "col", split_axis=0, concat_axis=0, tiled=True)
        outs.append(jnp.einsum("edszg,sdkmzf->gmkef", z_table, levels, precision=high))
    whole = jnp.concatenate(outs, axis=2) if pieces > 1 else outs[0]
    local_q = 2 * waves
    whole = whole.reshape(depth, members, local_q, local_y)
    return whole


def per_device(field, modes):
    rows, cols = lax.axis_size("row"), lax.axis_size("col")
    plan = Plan(field.shape, rows, cols)
    members, depth, waves, local_y = plan.members, plan.depth, plan.waves, plan.local_y
    whole = exchanged(plan, field, 1.0 / math.sqrt(NX * NY * NZ)) if plan.fits() else general(field)
    spectrum = jnp.transpose(whole, (0, 3, 1, 2))
    row_start = lax.axis_index("row") * waves
    col_start = lax.axis_index("col") * local_y
    wave = modes[0] - row_start
    line = modes[1] - col_start
    inside = (wave >= 0) & (wave < waves) & (line >= 0) & (line < local_y)
    wave = jnp.clip(wave, 0, waves - 1)
    line = jnp.clip(line, 0, local_y - 1)
    columns = lax.iota(jnp.int32, local_y)
    tall = whole.reshape(depth, members, waves, 2, local_y)
    picked = tall[modes[2], :, wave]
    hit = (columns[None, :] == line[:, None]) & inside[:, None]
    value = jnp.sum(jnp.where(hit[:, None, None, :], picked, 0.0), axis=-1)
    partial_value = jnp.transpose(value, (1, 2, 0)).reshape(members, -1)
    coef = lax.psum(partial_value, ("row", "col"))
    anomaly = coef - jnp.mean(coef, axis=0, keepdims=True)
    cov = jnp.dot(anomaly.T, anomaly, precision=highest) / (members - 1)
    localized = cov * taper_of(modes, NY, NZ, REACH)
    return (spectrum, localized)


def solution(mesh):
    placed = (P("row", "col", None, None), P())
    return jax.shard_map(
        per_device,
        mesh=mesh,
        in_specs=placed,
        out_specs=(P(None, "col", None, "row"), P()),
        check_vma=False,
    )
```

```python
import functools
import math

import jax
import jax.numpy as jnp
import numpy as np
from jax import lax
from jax.experimental import pallas as pl
from jax.experimental.pallas import tpu as pltpu
from jax.experimental.layout import Layout, with_layout_constraint
from jax.sharding import PartitionSpec as P

NX = 512
NY = 512
NZ = 64
REACH = 64


highest = lax.Precision.HIGHEST
high = lax.Precision.HIGH
PIECES = 2


def tables(length, count):
    points = lax.iota(jnp.int32, length)
    waves = lax.iota(jnp.int32, count)
    phase = points[:, None] * waves[None, :] % length
    angle = phase.astype(jnp.float32) * (2.0 * math.pi / length)
    return (jnp.cos(angle), jnp.sin(angle))


def taper_of(modes, size_y, size_z, reach):
    first = modes[0].astype(jnp.float32)
    second = jnp.where(modes[1] < size_y // 2, modes[1], modes[1] - size_y).astype(jnp.float32)
    third = jnp.where(modes[2] < size_z // 2, modes[2], modes[2] - size_z).astype(jnp.float32)
    first = jnp.concatenate([first, first])
    second = jnp.concatenate([second, second])
    third = jnp.concatenate([third, third])
    dist = (first[:, None] - first[None, :]) ** 2 + (second[:, None] - second[None, :]) ** 2
    dist = dist + (third[:, None] - third[None, :]) ** 2
    return jnp.exp(-dist / (2.0 * reach * reach))


def twiddle(length, count, scale):
    cos, sin = tables(length, count)
    cos, sin = cos * scale, sin * scale
    return jnp.stack([jnp.stack([cos, sin]), jnp.stack([-sin, cos])])


MESH = pl.DeviceIdType.MESH
LANES = 128
LIMIT = 49000000
SUB = 8


def split(value):
    top = value.astype(jnp.bfloat16)
    rest = (value - top.astype(jnp.float32)).astype(jnp.bfloat16)
    return top, rest


def waves_of(length, scale):
    j = np.arange(length)
    coarse = 2.0 * np.pi * (np.arange(0, length, SUB)[:, None] * j[None, :] % length) / length
    fine = 2.0 * np.pi * (np.arange(SUB)[:, None] * j[None, :] % length) / length
    coarse = np.stack([np.cos(coarse), np.sin(coarse)]) * scale
    fine = np.stack([np.cos(fine), np.sin(fine)])
    return coarse.astype(np.float32), fine.astype(np.float32)


def cmul(a, c, s):
    re, im = a
    if c == 1.0 and s == 0.0:
        return a
    if c == 0.0 and s == 1.0:
        return im, -re
    return re * c + im * s, im * c - re * s


def fft(items):
    n = len(items)
    if n == 1:
        return items
    even, odd = fft(items[0::2]), fft(items[1::2])
    out = [None] * n
    for k in range(n // 2):
        er, ei = even[k]
        if 8 * k == n or 8 * k == 3 * n:
            r, i = odd[k]
            h = math.sqrt(0.5)
            if 8 * k == n:
                tr, ti = (r + i) * h, (i - r) * h
            else:
                tr, ti = (i - r) * h, (r + i) * (-h)
        elif k == 0:
            tr, ti = odd[k]
        elif 4 * k == n:
            tr, ti = odd[k][1], None
        else:
            angle = 2.0 * math.pi * k / n
            tr, ti = cmul(odd[k], math.cos(angle), math.sin(angle))
        if ti is None:
            r = odd[k][0]
            out[k] = (er + tr, ei - r)
            out[k + n // 2] = (er - tr, ei + r)
        else:
            out[k] = (er + tr, ei + ti)
            out[k + n // 2] = (er - tr, ei - ti)
    return out


class Plan:
    def __init__(self, shape, rows, cols):
        self.near, self.thick, self.members, self.width = shape
        self.rows, self.cols = rows, cols
        self.length = self.near * rows
        self.depth = self.thick * cols
        self.waves = self.width // 2 // rows
        self.local_y = self.length // cols
        self.parts = self.waves // SUB
        self.pieces = self.members * self.parts
        self.lanes = self.near * self.thick
        self.tiles = self.lanes // LANES
        self.slabs = rows * self.tiles

    def fits(self):
        def power(n):
            return n > 1 and n & (n - 1) == 0

        return (
            power(self.rows)
            and power(self.cols)
            and self.waves % SUB == 0
            and self.near * 2 == LANES
            and self.local_y == LANES
            and self.thick % 4 == 0
            and self.rows % 2 == 0
            and self.slabs == self.cols * self.thick
            and self.depth == 64
            and self.width % 256 == 0
            and self.width == self.length
            and power(self.length)
            and self.members == SUB
        )


def kernel(
    plan, factor, field, modes, coarse, fine, D, localized,
    A, B, xtab, ytab, ptab, lines, mid, part, subtotal, col_parts, row_parts,
    row_send, row_recv, col_send, col_recv, in_sem, sum_send, sum_col, sum_row,
):
    R, C, H, T = plan.rows, plan.cols, plan.parts, plan.tiles
    near, thick = plan.near, plan.thick
    row, col = lax.axis_index("row"), lax.axis_index("col")

    def row_peer(k):
        return (row ^ k, col)

    def col_peer(k):
        return (row, col ^ k)

    row_order = list(range(R // 2, R)) + list(range(1, R // 2))
    col_order = list(range(C // 2, C)) + list(range(1, C // 2))

    def load(m, slot):
        return [
            pltpu.make_async_copy(field.at[:, z, m, :], lines.at[slot, pl.ds(z * near, near), :], in_sem.at[slot])
            for z in range(thick)
        ]

    for copy in load(0, 0):
        copy.start()

    barrier = pltpu.get_barrier_semaphore()
    for k in range(1, R):
        pl.semaphore_signal(barrier, inc=1, device_id=row_peer(k), device_id_type=MESH)
    for k in range(1, C):
        pl.semaphore_signal(barrier, inc=1, device_id=col_peer(k), device_id_type=MESH)

    fc, fs = fine[0], fine[1]

    def x_rows(i, _):
        h, r = i // R, i % R
        a = r * H + h
        uc, us = coarse[0, pl.ds(a, 1), :], coarse[1, pl.ds(a, 1), :]
        block = jnp.concatenate([uc * fc - us * fs, -(us * fc + uc * fs)], axis=0)
        top, rest = split(block)
        at = pl.ds(pl.multiple_of(i * 2 * SUB, 2 * SUB), 2 * SUB)
        xtab[0, at, :] = top
        xtab[1, at, :] = rest
        return 0

    lax.fori_loop(0, H * R, x_rows, 0)

    pl.semaphore_wait(barrier, R + C - 2)

    def row_copy(p, k):
        return pltpu.make_async_remote_copy(
            A.at[p, pl.ds((row ^ k) * T, T)],
            B.at[p, pl.ds(row * T, T)],
            row_send.at[p],
            row_recv.at[p, k],
            device_id=row_peer(k),
            device_id_type=MESH,
        )

    def row_wait(p, k):
        return pltpu.make_async_remote_copy(
            A.at[p, pl.ds((row ^ k) * T, T)],
            B.at[p, pl.ds((row ^ k) * T, T)],
            row_send.at[p],
            row_recv.at[p, k],
            device_id=row_peer(k),
            device_id_type=MESH,
        )

    def col_copy(p, k):
        return pltpu.make_async_remote_copy(
            A.at[p, pl.ds((col ^ k) * thick, thick)],
            D.at[p, pl.ds(col * thick, thick)],
            col_send.at[p],
            col_recv.at[p, k],
            device_id=col_peer(k),
            device_id_type=MESH,
        )

    def col_wait(p, k):
        return pltpu.make_async_remote_copy(
            A.at[p, pl.ds((col ^ k) * thick, thick)],
            D.at[p, pl.ds((col ^ k) * thick, thick)],
            col_send.at[p],
            col_recv.at[p, k],
            device_id=col_peer(k),
            device_id_type=MESH,
        )

    def contract(a, b):
        return lax.dot_general(a, b, (((1,), (1,)), ((), ())), preferred_element_type=jnp.float32)

    chunk = 2 * LANES

    for m in range(plan.members):
        slot = m % 2
        if m + 1 < plan.members:
            for copy in load(m + 1, 1 - slot):
                copy.start()
        for copy in load(m, slot):
            copy.wait()

        def x_step(g, _):
            at = pl.ds(pl.multiple_of(g * chunk, chunk), chunk)
            top, rest = split(lines[slot, at, :])
            got = contract(xtab[0], top) + (contract(xtab[0], rest) + contract(xtab[1], top))
            for h in range(H):
                for r in range(R):
                    base = (h * R + r) * 2 * SUB
                    for t in range(chunk // LANES):
                        A[m * H + h, r * T + g * (chunk // LANES) + t] = got[base : base + 2 * SUB, t * LANES : (t + 1) * LANES]
            return 0

        lax.fori_loop(0, plan.lanes // chunk, x_step, 0)
        for h in range(H):
            p = m * H + h
            mine = pl.ds(row * T, T)
            B[p, mine] = A[p, mine]
            for k in row_order:
                row_copy(p, k).start()

    count = modes.shape[1]
    pick_x, pick_y, pick_z = modes[0:1, :], modes[1:2, :], modes[2:3, :]

    def phase_rows(t, _):
        cell = t * LANES + lax.broadcasted_iota(jnp.int32, (LANES, count), 0)
        y = row * near + cell % near
        z = col * thick + cell // near
        turns = (pick_y * y + (plan.length // plan.depth) * pick_z * z) % plan.length
        half = (turns - plan.length // 2).astype(jnp.float32) * (math.pi / plan.length)
        square = half * half
        sine, cosine = 1.0, 1.0
        for n in range(6, 0, -1):
            sine = 1.0 - square * sine * (1.0 / (2 * n * (2 * n + 1)))
        for n in range(7, 0, -1):
            cosine = 1.0 - square * cosine * (1.0 / (2 * n * (2 * n - 1)))
        sine = half * sine
        top, rest = split(jnp.concatenate([2.0 * sine * sine - 1.0, -2.0 * sine * cosine], axis=1))
        at = pl.ds(pl.multiple_of(t * LANES, LANES), LANES)
        ptab[0, at, :] = top
        ptab[1, at, :] = rest
        return 0

    lax.fori_loop(0, plan.lanes // LANES, phase_rows, 0)
    part[...] = jnp.zeros_like(part)
    owner = lax.broadcasted_iota(jnp.int32, (R, SUB, count), 0)
    inner = lax.broadcasted_iota(jnp.int32, (R, SUB, count), 1)

    def part_step(p, _):
        m, h = p // H, p % H
        cells = jnp.concatenate(
            [jnp.concatenate([A[p, r * T + t] for t in range(T)], axis=1) for r in range(R)], axis=0
        )
        top, rest = split(cells)

        def times(a, b):
            return jnp.dot(a, b, preferred_element_type=jnp.float32)

        got = times(top, ptab[0]) + (times(rest, ptab[0]) + times(top, ptab[1]))
        got = got.reshape(R, 2, SUB, 2 * count)
        re = got[:, 0, :, :count] + got[:, 1, :, count:]
        im = got[:, 1, :, :count] - got[:, 0, :, count:]
        hit = owner * plan.waves + h * SUB + inner == pick_x.reshape(1, 1, count)
        for c, value in enumerate((re, im)):
            found = jnp.sum(jnp.where(hit, value, 0.0), axis=(0, 1)).reshape(1, count)
            at = slice(c * count, (c + 1) * count)
            part[pl.ds(m, 1), at] = part[pl.ds(m, 1), at] + found
        return 0

    lax.fori_loop(0, plan.pieces, part_step, 0)
    col_parts[col] = part[...]

    def col_sum(k):
        return pltpu.make_async_remote_copy(
            part, col_parts.at[col], sum_send.at[0], sum_col.at[k], device_id=col_peer(k), device_id_type=MESH
        )

    def col_sum_wait(k):
        return pltpu.make_async_remote_copy(
            part, col_parts.at[col ^ k], sum_send.at[0], sum_col.at[k], device_id=col_peer(k), device_id_type=MESH
        )

    def row_sum(k):
        return pltpu.make_async_remote_copy(
            subtotal, row_parts.at[row], sum_send.at[1], sum_row.at[k], device_id=row_peer(k), device_id_type=MESH
        )

    def row_sum_wait(k):
        return pltpu.make_async_remote_copy(
            subtotal, row_parts.at[row ^ k], sum_send.at[1], sum_row.at[k], device_id=row_peer(k), device_id_type=MESH
        )

    for k in col_order:
        col_sum(k).start()

    length = plan.length

    def y_rows(i, _):
        blocks = []
        for b in range(2):
            a = 2 * i + b
            uc, us = coarse[0, pl.ds(a, 1), :], coarse[1, pl.ds(a, 1), :]
            blocks.append(jnp.concatenate([uc * fc - us * fs, us * fc + uc * fs], axis=1))
        top, rest = split(jnp.concatenate(blocks, axis=0) * factor)
        at = pl.ds(pl.multiple_of(i * 2 * SUB, 2 * SUB), 2 * SUB)
        ytab[0, at, :] = top
        ytab[1, at, :] = rest
        return 0

    lax.fori_loop(0, length // (2 * SUB), y_rows, 0)

    for k in col_order:
        col_sum_wait(k).wait_recv()
    total = col_parts[0]
    for c in range(1, C):
        total = total + col_parts[c]
    subtotal[...] = total
    row_parts[row] = total
    for k in row_order:
        row_sum(k).start()

    low = lax.broadcasted_iota(jnp.int32, (T * 2 * SUB, LANES), 1) < near

    def y_step(p):
        evens, odds = [], []
        for t in range(R // 2):
            v0 = B[p, 2 * t * T : (2 * t + 1) * T].reshape(T * 2 * SUB, LANES)
            v1 = B[p, (2 * t + 1) * T : (2 * t + 2) * T].reshape(T * 2 * SUB, LANES)
            evens.append(jnp.where(low, v0, pltpu.roll(v1, near, 1)))
            odds.append(jnp.where(low, pltpu.roll(v0, near, 1), v1))
        left = jnp.concatenate([jnp.concatenate(evens, axis=1), jnp.concatenate(odds, axis=1)], axis=0)
        top, rest = split(left)

        def times(a, b):
            return jnp.dot(a, b, preferred_element_type=jnp.float32)

        for c in range(C):
            at_c = slice(c * LANES, (c + 1) * LANES)
            at_s = slice(length + c * LANES, length + (c + 1) * LANES)

            def product(at):
                return times(top, ytab[0, :, at]) + (times(rest, ytab[0, :, at]) + times(top, ytab[1, :, at]))

            both = product(at_c).reshape(thick, 2, SUB, LANES), product(at_s).reshape(thick, 2, SUB, LANES)
            re = both[0][:, 0] + both[1][:, 1]
            im = both[0][:, 1] - both[1][:, 0]
            A[p, c * thick : (c + 1) * thick, 0:SUB] = re
            A[p, c * thick : (c + 1) * thick, SUB : 2 * SUB] = im

    def slab(z):
        inner = z % thick
        return z // thick * thick + inner % 2 * (thick // 2) + inner // 2

    eight = 8

    def z_step(p):
        for z0 in range(eight):
            items = []
            for z1 in range(eight):
                at = slab(z1 * eight + z0)
                items.append((D[p, at, 0:SUB], D[p, at, SUB : 2 * SUB]))
            for k0, value in enumerate(fft(items)):
                angle = 2.0 * math.pi * z0 * k0 / 64
                re, im = value if z0 * k0 == 0 else cmul(value, math.cos(angle), math.sin(angle))
                mid[k0 * eight + z0, 0:SUB] = re
                mid[k0 * eight + z0, SUB : 2 * SUB] = im
        for k0 in range(eight):
            items = []
            for z0 in range(eight):
                at = k0 * eight + z0
                items.append((mid[at, 0:SUB], mid[at, SUB : 2 * SUB]))
            for k1, (re, im) in enumerate(fft(items)):
                D[p, k0 + eight * k1, pl.ds(0, SUB, stride=2), :] = re
                D[p, k0 + eight * k1, pl.ds(1, SUB, stride=2), :] = im

    def finish(p):
        for k in col_order:
            col_wait(p, k).wait_recv()
        z_step(p)

    def step(p, _):
        for k in row_order:
            row_wait(p, k).wait_recv()
        for k in row_order:
            row_wait(p, k).wait_send()
        y_step(p)
        mine = pl.ds(col * thick, thick)
        D[p, mine] = A[p, mine]
        for k in col_order:
            col_copy(p, k).start()

        @pl.when(p >= 1)
        def _():
            finish(p - 1)

        return 0

    def localize():
        for k in row_order:
            row_sum_wait(k).wait_recv()
        total = row_parts[0]
        for r in range(1, R):
            total = total + row_parts[r]
        coef = total * factor
        anomaly = coef - jnp.sum(coef, axis=0, keepdims=True) / plan.members
        columns = 2 * count

        def signed(wave, size):
            return jnp.where(wave < size // 2, wave, wave - size).astype(jnp.float32)

        places = [pick_x.astype(jnp.float32), signed(pick_y, plan.length), signed(pick_z, plan.depth)]
        places = [jnp.concatenate([place, place], axis=1) for place in places]
        squares = places[0] * places[0] + places[1] * places[1] + places[2] * places[2]
        ones = jnp.ones_like(squares)
        nothing = jnp.zeros((LANES - 5, columns), jnp.float32)
        left = jnp.concatenate(places + [squares, ones, nothing], axis=0)
        right = jnp.concatenate([-2.0 * place for place in places] + [ones, squares, nothing], axis=0)
        padded = jnp.concatenate([anomaly, jnp.zeros((LANES - plan.members, columns), jnp.float32)], axis=0)
        left, turned = jnp.transpose(left), jnp.transpose(padded)

        def times(a, b):
            return jnp.dot(a, b, precision=highest, preferred_element_type=jnp.float32)

        for i in range(0, columns, LANES):
            cov = times(turned[i : i + LANES], padded) / (plan.members - 1)
            dist = times(left[i : i + LANES], right)
            localized[i : i + LANES, :] = cov * jnp.exp(-dist / (2.0 * REACH * REACH))

    lax.fori_loop(0, plan.pieces, step, 0)
    localize()
    finish(plan.pieces - 1)
    def drain(p, _):
        for k in col_order:
            col_copy(p, k).wait_send()
        return 0

    lax.fori_loop(0, plan.pieces, drain, 0)
    for k in col_order:
        col_sum(k).wait_send()
    for k in row_order:
        row_sum(k).wait_send()


def exchanged(plan, field, modes, factor):
    coarse, fine = waves_of(plan.length, 1.0)
    count = modes.shape[1]
    sums = (plan.members, 2 * count)
    block = (plan.pieces, plan.slabs, 2 * SUB, LANES)
    return pl.pallas_call(
        functools.partial(kernel, plan, factor),
        out_shape=(
            pltpu.VMEM(block, jnp.float32),
            pltpu.VMEM((2 * count, 2 * count), jnp.float32),
        ),
        in_specs=[
            pl.BlockSpec(memory_space=pl.ANY),
            pl.BlockSpec(memory_space=pltpu.VMEM),
            pl.BlockSpec(memory_space=pltpu.VMEM),
            pl.BlockSpec(memory_space=pltpu.VMEM),
        ],
        out_specs=(pl.BlockSpec(memory_space=pltpu.VMEM), pl.BlockSpec(memory_space=pltpu.VMEM)),
        scratch_shapes=[
            pltpu.VMEM(block, jnp.float32),
            pltpu.VMEM(block, jnp.float32),
            pltpu.VMEM((2, plan.width, plan.width), jnp.bfloat16),
            pltpu.VMEM((2, plan.length, 2 * plan.length), jnp.bfloat16),
            pltpu.VMEM((2, plan.lanes, 2 * count), jnp.bfloat16),
            pltpu.VMEM((2, plan.lanes, plan.width), jnp.float32),
            pltpu.VMEM((plan.depth, 2 * SUB, LANES), jnp.float32),
            pltpu.VMEM(sums, jnp.float32),
            pltpu.VMEM(sums, jnp.float32),
            pltpu.VMEM((plan.cols,) + sums, jnp.float32),
            pltpu.VMEM((plan.rows,) + sums, jnp.float32),
            pltpu.SemaphoreType.DMA((plan.pieces,)),
            pltpu.SemaphoreType.DMA((plan.pieces, plan.rows)),
            pltpu.SemaphoreType.DMA((plan.pieces,)),
            pltpu.SemaphoreType.DMA((plan.pieces, plan.cols)),
            pltpu.SemaphoreType.DMA((2,)),
            pltpu.SemaphoreType.DMA((2,)),
            pltpu.SemaphoreType.DMA((plan.cols,)),
            pltpu.SemaphoreType.DMA((plan.rows,)),
        ],
        compiler_params=pltpu.CompilerParams(collective_id=0, has_side_effects=True, vmem_limit_bytes=LIMIT),
    )(field, modes, jnp.asarray(coarse), jnp.asarray(fine))


def settle(plan, piled, square, whole, localized, sems):
    H = plan.parts
    copies = [pltpu.make_async_copy(square, localized, sems.at[plan.pieces])]
    for p in range(plan.pieces):
        m, h = p // H, p % H
        copies.append(pltpu.make_async_copy(piled.at[p], whole.at[:, m, pl.ds(h * 2 * SUB, 2 * SUB), :], sems.at[p]))
    for copy in copies:
        copy.start()
    for copy in copies:
        copy.wait()


def settled(plan, piled, square):
    return pl.pallas_call(
        functools.partial(settle, plan),
        out_shape=(
            jax.ShapeDtypeStruct((plan.depth, plan.members, 2 * plan.waves, plan.local_y), jnp.float32),
            jax.ShapeDtypeStruct(square.shape, jnp.float32),
        ),
        in_specs=[pl.BlockSpec(memory_space=pltpu.VMEM), pl.BlockSpec(memory_space=pltpu.VMEM)],
        out_specs=(pl.BlockSpec(memory_space=pl.ANY), pl.BlockSpec(memory_space=pl.ANY)),
        scratch_shapes=[pltpu.SemaphoreType.DMA((plan.pieces + 1,))],
        compiler_params=pltpu.CompilerParams(vmem_limit_bytes=1 << 20),
    )(pltpu.with_memory_space_constraint(piled, pltpu.VMEM), pltpu.with_memory_space_constraint(square, pltpu.VMEM))


def general(field):
    members = field.shape[2]
    width = field.shape[3]
    rows, cols = lax.axis_size("row"), lax.axis_size("col")
    near, thick = field.shape[0], field.shape[1]
    length, depth = near * rows, thick * cols
    waves = width // 2 // rows
    pieces = PIECES if waves % PIECES == 0 else 1
    part = waves // pieces
    local_y = length // cols
    factor = 1.0 / math.sqrt(NX * NY * NZ)
    cos_x, sin_x = tables(width, width // 2)
    x_table = jnp.stack([cos_x, -sin_x]).reshape(2, width, rows, pieces, part)
    y_table = twiddle(length, length, 1.0).reshape(2, 2, rows, near, length)
    z_table = twiddle(depth, depth, factor).reshape(2, 2, cols, thick, depth)
    flat = field.reshape(near, thick * members, width)
    outs = []
    for piece in range(pieces):
        lines = jnp.einsum("cxrk,ylx->rckyl", x_table[:, :, :, piece], flat, precision=high)
        lines = with_layout_constraint(lines, Layout((0, 1, 2, 3, 4)))
        gathered = lax.all_to_all(lines, "row", split_axis=0, concat_axis=0, tiled=True)
        gathered = with_layout_constraint(gathered, Layout((0, 1, 2, 3, 4)))
        gathered = gathered.reshape(rows, 2, part, near, thick, members)
        ytrans = jnp.einsum("dcsyf,sckyzm->dkmzf", y_table, gathered, precision=high)
        ytrans = ytrans.reshape(2, part, members, thick, cols, local_y)
        ytrans = jnp.transpose(ytrans, (4, 0, 1, 2, 3, 5))
        levels = lax.all_to_all(ytrans, "col", split_axis=0, concat_axis=0, tiled=True)
        outs.append(jnp.einsum("edszg,sdkmzf->gmkef", z_table, levels, precision=high))
    whole = jnp.concatenate(outs, axis=2) if pieces > 1 else outs[0]
    local_q = 2 * waves
    whole = whole.reshape(depth, members, local_q, local_y)
    return whole


def general_localized(whole, modes):
    rows, cols = lax.axis_size("row"), lax.axis_size("col")
    depth, members, local_q, local_y = whole.shape
    waves = local_q // 2
    row_start = lax.axis_index("row") * waves
    col_start = lax.axis_index("col") * local_y
    wave = modes[0] - row_start
    line = modes[1] - col_start
    inside = (wave >= 0) & (wave < waves) & (line >= 0) & (line < local_y)
    wave = jnp.clip(wave, 0, waves - 1)
    line = jnp.clip(line, 0, local_y - 1)
    columns = lax.iota(jnp.int32, local_y)
    tall = whole.reshape(depth, members, waves, 2, local_y)
    picked = tall[modes[2], :, wave]
    hit = (columns[None, :] == line[:, None]) & inside[:, None]
    value = jnp.sum(jnp.where(hit[:, None, None, :], picked, 0.0), axis=-1)
    partial_value = jnp.transpose(value, (1, 2, 0)).reshape(members, -1)
    coef = lax.psum(partial_value, ("row", "col"))
    anomaly = coef - jnp.mean(coef, axis=0, keepdims=True)
    cov = jnp.dot(anomaly.T, anomaly, precision=highest) / (members - 1)
    localized = cov * taper_of(modes, NY, NZ, REACH)
    return localized


def per_device(field, modes):
    plan = Plan(field.shape, lax.axis_size("row"), lax.axis_size("col"))
    factor = 1.0 / math.sqrt(NX * NY * NZ)
    if plan.fits() and modes.shape[1] % LANES == 0:
        whole, localized = settled(plan, *exchanged(plan, field, modes, factor))
    else:
        whole = general(field)
        localized = general_localized(whole, modes)
    return (jnp.transpose(whole, (0, 3, 1, 2)), localized)


def solution(mesh):
    placed = (P("row", "col", None, None), P())
    return jax.shard_map(
        per_device,
        mesh=mesh,
        in_specs=placed,
        out_specs=(P(None, "col", None, "row"), P()),
        check_vma=False,
    )
```

```python
import functools
import math

import jax
import jax.numpy as jnp
import numpy as np
from jax import lax
from jax.experimental import pallas as pl
from jax.experimental.pallas import tpu as pltpu
from jax.experimental.layout import Layout, with_layout_constraint
from jax.sharding import PartitionSpec as P

NX = 512
NY = 512
NZ = 64
REACH = 64


highest = lax.Precision.HIGHEST
high = lax.Precision.HIGH
PIECES = 2


def tables(length, count):
    points = lax.iota(jnp.int32, length)
    waves = lax.iota(jnp.int32, count)
    phase = points[:, None] * waves[None, :] % length
    angle = phase.astype(jnp.float32) * (2.0 * math.pi / length)
    return (jnp.cos(angle), jnp.sin(angle))


def taper_of(modes, size_y, size_z, reach):
    first = modes[0].astype(jnp.float32)
    second = jnp.where(modes[1] < size_y // 2, modes[1], modes[1] - size_y).astype(jnp.float32)
    third = jnp.where(modes[2] < size_z // 2, modes[2], modes[2] - size_z).astype(jnp.float32)
    first = jnp.concatenate([first, first])
    second = jnp.concatenate([second, second])
    third = jnp.concatenate([third, third])
    dist = (first[:, None] - first[None, :]) ** 2 + (second[:, None] - second[None, :]) ** 2
    dist = dist + (third[:, None] - third[None, :]) ** 2
    return jnp.exp(-dist / (2.0 * reach * reach))


def twiddle(length, count, scale):
    cos, sin = tables(length, count)
    cos, sin = cos * scale, sin * scale
    return jnp.stack([jnp.stack([cos, sin]), jnp.stack([-sin, cos])])


MESH = pl.DeviceIdType.MESH
LANES = 128
LIMIT = 49000000
SUB = 8


def split(value):
    top = value.astype(jnp.bfloat16)
    rest = (value - top.astype(jnp.float32)).astype(jnp.bfloat16)
    return top, rest


def waves_of(length, scale):
    j = np.arange(length)
    coarse = 2.0 * np.pi * (np.arange(0, length, SUB)[:, None] * j[None, :] % length) / length
    fine = 2.0 * np.pi * (np.arange(SUB)[:, None] * j[None, :] % length) / length
    coarse = np.stack([np.cos(coarse), np.sin(coarse)]) * scale
    fine = np.stack([np.cos(fine), np.sin(fine)])
    return coarse.astype(np.float32), fine.astype(np.float32)


def cmul(a, c, s):
    re, im = a
    if c == 1.0 and s == 0.0:
        return a
    if c == 0.0 and s == 1.0:
        return im, -re
    return re * c + im * s, im * c - re * s


def fft(items):
    n = len(items)
    if n == 1:
        return items
    even, odd = fft(items[0::2]), fft(items[1::2])
    out = [None] * n
    for k in range(n // 2):
        er, ei = even[k]
        if 8 * k == n or 8 * k == 3 * n:
            r, i = odd[k]
            h = math.sqrt(0.5)
            if 8 * k == n:
                tr, ti = (r + i) * h, (i - r) * h
            else:
                tr, ti = (i - r) * h, (r + i) * (-h)
        elif k == 0:
            tr, ti = odd[k]
        elif 4 * k == n:
            tr, ti = odd[k][1], None
        else:
            angle = 2.0 * math.pi * k / n
            tr, ti = cmul(odd[k], math.cos(angle), math.sin(angle))
        if ti is None:
            r = odd[k][0]
            out[k] = (er + tr, ei - r)
            out[k + n // 2] = (er - tr, ei + r)
        else:
            out[k] = (er + tr, ei + ti)
            out[k + n // 2] = (er - tr, ei - ti)
    return out


class Plan:
    def __init__(self, shape, rows, cols):
        self.near, self.thick, self.members, self.width = shape
        self.rows, self.cols = rows, cols
        self.length = self.near * rows
        self.depth = self.thick * cols
        self.waves = self.width // 2 // rows
        self.local_y = self.length // cols
        self.parts = self.waves // SUB
        self.pieces = self.members * self.parts
        self.lanes = self.near * self.thick
        self.tiles = self.lanes // LANES
        self.slabs = rows * self.tiles
        self.groups = 4

    def fits(self):
        def power(n):
            return n > 1 and n & (n - 1) == 0

        return (
            power(self.rows)
            and power(self.cols)
            and self.waves % SUB == 0
            and self.near * 2 == LANES
            and self.local_y == LANES
            and self.thick % (2 * self.groups) == 0
            and self.members >= 3
            and self.rows % 2 == 0
            and self.slabs == self.cols * self.thick
            and self.depth == 64
            and self.width % 256 == 0
            and self.width == self.length
            and power(self.length)
            and self.members == SUB
        )


def kernel(
    plan, factor, field, modes_in, coarse_in, fine_in, D, localized,
    A, B, last, xtab, ytab, ptab, lines, mid, modes, coarse, fine, part, subtotal, col_parts, row_parts,
    row_send, row_recv, col_send, col_recv, in_sem, table_sem, sum_send, sum_col, sum_row,
):
    R, C, H, T = plan.rows, plan.cols, plan.parts, plan.tiles
    near, thick, groups = plan.near, plan.thick, plan.groups
    ply, deep = T // groups, thick // groups
    final = plan.pieces - 1
    row, col = lax.axis_index("row"), lax.axis_index("col")

    def row_peer(k):
        return (row ^ k, col)

    def col_peer(k):
        return (row, col ^ k)

    row_order = list(range(R // 2, R)) + list(range(1, R // 2))
    col_order = list(range(C // 2, C)) + list(range(1, C // 2))

    def load(m, z, sem):
        at = pl.ds(pl.multiple_of(z * near, near), near)
        return pltpu.make_async_copy(field.at[:, z, m, :], lines.at[m % 2, at, :], in_sem.at[sem])

    tables = [
        pltpu.make_async_copy(coarse_in, coarse, table_sem.at[0]),
        pltpu.make_async_copy(fine_in, fine, table_sem.at[1]),
        pltpu.make_async_copy(modes_in, modes, table_sem.at[2]),
    ]
    for copy in tables:
        copy.start()
    for z in range(thick):
        load(0, z, z // deep).start()

    barrier = pltpu.get_barrier_semaphore()
    for k in range(1, R):
        pl.semaphore_signal(barrier, inc=1, device_id=row_peer(k), device_id_type=MESH)
    for k in range(1, C):
        pl.semaphore_signal(barrier, inc=1, device_id=col_peer(k), device_id_type=MESH)
    for copy in tables:
        copy.wait()

    fc, fs = fine[0], fine[1]

    def x_rows(i, _):
        h, r = i // R, i % R
        a = r * H + h
        uc, us = coarse[0, pl.ds(a, 1), :], coarse[1, pl.ds(a, 1), :]
        block = jnp.concatenate([uc * fc - us * fs, -(us * fc + uc * fs)], axis=0)
        top, rest = split(block)
        at = pl.ds(pl.multiple_of(i * 2 * SUB, 2 * SUB), 2 * SUB)
        xtab[0, at, :] = top
        xtab[1, at, :] = rest
        return 0

    lax.fori_loop(0, H * R, x_rows, 0)

    pl.semaphore_wait(barrier, R + C - 2)

    def row_copy(src, dst, unit, k):
        return pltpu.make_async_remote_copy(
            src, dst, row_send.at[unit], row_recv.at[unit, k], device_id=row_peer(k), device_id_type=MESH
        )

    def row_part(p, k, unit, first=0, size=T):
        return row_copy(
            A.at[p, pl.ds((row ^ k) * T + first, size)], B.at[p, pl.ds(row * T + first, size)], unit, k
        )

    def row_wait(p, k, unit, first=0, size=T):
        return row_copy(
            A.at[p, pl.ds((row ^ k) * T + first, size)], B.at[p, pl.ds((row ^ k) * T + first, size)], unit, k
        )

    def col_copy(src, dst, unit, k):
        return pltpu.make_async_remote_copy(
            src, dst, col_send.at[unit], col_recv.at[unit, k], device_id=col_peer(k), device_id_type=MESH
        )

    def col_part(out, p, k, unit, first=0, size=thick):
        return col_copy(
            out.at[pl.ds((col ^ k) * thick + first, size)], D.at[p, pl.ds(col * thick + first, size)], unit, k
        )

    def col_wait(out, p, k, unit, first=0, size=thick):
        return col_copy(
            out.at[pl.ds((col ^ k) * thick + first, size)], D.at[p, pl.ds((col ^ k) * thick + first, size)], unit, k
        )

    def contract(a, b):
        return lax.dot_general(a, b, (((1,), (1,)), ((), ())), preferred_element_type=jnp.float32)

    chunk = ply * LANES

    def x_step(m, g):
        at = pl.ds(pl.multiple_of(g * chunk, chunk), chunk)
        top, rest = split(lines[m % 2, at, :])
        got = contract(xtab[0], top) + (contract(xtab[0], rest) + contract(xtab[1], top))
        for h in range(H):
            for r in range(R):
                base = (h * R + r) * 2 * SUB
                for t in range(ply):
                    A[m * H + h, r * T + g * ply + t] = got[base : base + 2 * SUB, t * LANES : (t + 1) * LANES]

    mine = pl.ds(row * T, T)

    def x_first(g, _):
        for z in range(deep):
            load(0, g * deep + z, g).wait()
        x_step(0, g)
        for k in row_order:
            row_copy(
                A.at[pl.ds(0, H), pl.ds((row ^ k) * T + g * ply, ply)],
                B.at[pl.ds(0, H), pl.ds(row * T + g * ply, ply)],
                0,
                k,
            ).start()
        return 0

    lax.fori_loop(0, groups, x_first, 0)
    for z in range(thick):
        load(1, z, groups + 1).start()
    for h in range(H):
        B[h, mine] = A[h, mine]

    for m in range(1, plan.members):
        if m + 1 < plan.members:
            for z in range(thick):
                load(m + 1, z, groups + (m + 1) % 2).start()
        for z in range(thick):
            load(m, z, groups + m % 2).wait()

        def x_more(g, _):
            x_step(m, g)
            return 0

        lax.fori_loop(0, groups, x_more, 0)
        for h in range(H):
            p = m * H + h
            B[p, mine] = A[p, mine]
            if p < final:
                for k in row_order:
                    row_part(p, k, p).start()
            else:
                for g in range(groups):
                    for k in row_order:
                        row_part(final, k, final + g, g * ply, ply).start()

    count = modes.shape[1]
    pick_x, pick_y, pick_z = modes[0:1, :], modes[1:2, :], modes[2:3, :]

    def phase_rows(t, _):
        cell = t * LANES + lax.broadcasted_iota(jnp.int32, (LANES, count), 0)
        y = row * near + cell % near
        z = col * thick + cell // near
        turns = (pick_y * y + (plan.length // plan.depth) * pick_z * z) % plan.length
        half = (turns - plan.length // 2).astype(jnp.float32) * (math.pi / plan.length)
        square = half * half
        sine, cosine = 1.0, 1.0
        for n in range(6, 0, -1):
            sine = 1.0 - square * sine * (1.0 / (2 * n * (2 * n + 1)))
        for n in range(7, 0, -1):
            cosine = 1.0 - square * cosine * (1.0 / (2 * n * (2 * n - 1)))
        sine = half * sine
        top, rest = split(jnp.concatenate([2.0 * sine * sine - 1.0, -2.0 * sine * cosine], axis=1))
        at = pl.ds(pl.multiple_of(t * LANES, LANES), LANES)
        ptab[0, at, :] = top
        ptab[1, at, :] = rest
        return 0

    lax.fori_loop(0, plan.lanes // LANES, phase_rows, 0)
    part[...] = jnp.zeros_like(part)
    owner = lax.broadcasted_iota(jnp.int32, (R, SUB, count), 0)
    inner = lax.broadcasted_iota(jnp.int32, (R, SUB, count), 1)

    def part_step(p, _):
        m, h = p // H, p % H
        cells = jnp.concatenate(
            [jnp.concatenate([A[p, r * T + t] for t in range(T)], axis=1) for r in range(R)], axis=0
        )
        top, rest = split(cells)

        def times(a, b):
            return jnp.dot(a, b, preferred_element_type=jnp.float32)

        got = times(top, ptab[0]) + (times(rest, ptab[0]) + times(top, ptab[1]))
        got = got.reshape(R, 2, SUB, 2 * count)
        re = got[:, 0, :, :count] + got[:, 1, :, count:]
        im = got[:, 1, :, :count] - got[:, 0, :, count:]
        hit = owner * plan.waves + h * SUB + inner == pick_x.reshape(1, 1, count)
        for c, value in enumerate((re, im)):
            found = jnp.sum(jnp.where(hit, value, 0.0), axis=(0, 1)).reshape(1, count)
            at = slice(c * count, (c + 1) * count)
            part[pl.ds(m, 1), at] = part[pl.ds(m, 1), at] + found
        return 0

    lax.fori_loop(0, plan.pieces, part_step, 0)
    col_parts[col] = part[...]

    def col_sum(k):
        return pltpu.make_async_remote_copy(
            part, col_parts.at[col], sum_send.at[0], sum_col.at[k], device_id=col_peer(k), device_id_type=MESH
        )

    def col_sum_wait(k):
        return pltpu.make_async_remote_copy(
            part, col_parts.at[col ^ k], sum_send.at[0], sum_col.at[k], device_id=col_peer(k), device_id_type=MESH
        )

    def row_sum(k):
        return pltpu.make_async_remote_copy(
            subtotal, row_parts.at[row], sum_send.at[1], sum_row.at[k], device_id=row_peer(k), device_id_type=MESH
        )

    def row_sum_wait(k):
        return pltpu.make_async_remote_copy(
            subtotal, row_parts.at[row ^ k], sum_send.at[1], sum_row.at[k], device_id=row_peer(k), device_id_type=MESH
        )

    for k in col_order:
        col_sum(k).start()

    length = plan.length

    def y_rows(i, _):
        blocks = []
        for b in range(2):
            a = 2 * i + b
            uc, us = coarse[0, pl.ds(a, 1), :], coarse[1, pl.ds(a, 1), :]
            cosine, sine = uc * fc - us * fs, us * fc + uc * fs
            halves = []
            for c in range(C):
                at = slice(c * LANES, (c + 1) * LANES)
                halves += [cosine[:, at], sine[:, at]]
            blocks.append(jnp.concatenate(halves, axis=1))
        top, rest = split(jnp.concatenate(blocks, axis=0) * factor)
        at = pl.ds(pl.multiple_of(i * 2 * SUB, 2 * SUB), 2 * SUB)
        ytab[0, at, :] = top
        ytab[1, at, :] = rest
        return 0

    lax.fori_loop(0, length // (2 * SUB), y_rows, 0)

    for k in col_order:
        col_sum_wait(k).wait_recv()
    total = col_parts[0]
    for c in range(1, C):
        total = total + col_parts[c]
    subtotal[...] = total
    row_parts[row] = total
    for k in row_order:
        row_sum(k).start()


    def y_step(p, out, unit, first, size):
        low = lax.broadcasted_iota(jnp.int32, (size * 2 * SUB, LANES), 1) < near
        evens, odds = [], []
        for t in range(R // 2):
            v0 = B[p, 2 * t * T + first : 2 * t * T + first + size].reshape(size * 2 * SUB, LANES)
            v1 = B[p, (2 * t + 1) * T + first : (2 * t + 1) * T + first + size].reshape(size * 2 * SUB, LANES)
            evens.append(jnp.where(low, v0, pltpu.roll(v1, near, 1)))
            odds.append(jnp.where(low, pltpu.roll(v0, near, 1), v1))
        left = jnp.concatenate([jnp.concatenate(evens, axis=1), jnp.concatenate(odds, axis=1)], axis=0)
        top, rest = split(left)

        def times(a, b):
            return jnp.dot(a, b, preferred_element_type=jnp.float32)

        for k in col_order + [0]:
            c = col ^ k
            at = pl.ds(pl.multiple_of(c * 2 * LANES, 2 * LANES), 2 * LANES)
            both = times(top, ytab[0, :, at]) + (times(rest, ytab[0, :, at]) + times(top, ytab[1, :, at]))
            both = both.reshape(2, size, 2, SUB, 2 * LANES)
            re = both[:, :, 0, :, :LANES] + both[:, :, 1, :, LANES:]
            im = both[:, :, 1, :, :LANES] - both[:, :, 0, :, LANES:]
            for t in range(size):
                for odd in range(2):
                    z = c * thick + 2 * (first + t) + odd
                    if k == 0:
                        D[p, z, 0:SUB] = re[odd, t]
                        D[p, z, SUB : 2 * SUB] = im[odd, t]
                    else:
                        out[z, 0:SUB] = re[odd, t]
                        out[z, SUB : 2 * SUB] = im[odd, t]
            if k != 0:
                col_part(out, p, k, unit, 2 * first, 2 * size).start()

    eight = 8

    def z_step(p):
        for z0 in range(eight):
            items = []
            for z1 in range(eight):
                at = z1 * eight + z0
                items.append((D[p, at, 0:SUB], D[p, at, SUB : 2 * SUB]))
            for k0, value in enumerate(fft(items)):
                angle = 2.0 * math.pi * z0 * k0 / 64
                re, im = value if z0 * k0 == 0 else cmul(value, math.cos(angle), math.sin(angle))
                mid[k0 * eight + z0, 0:SUB] = re
                mid[k0 * eight + z0, SUB : 2 * SUB] = im
        for k0 in range(eight):
            items = []
            for z0 in range(eight):
                at = k0 * eight + z0
                items.append((mid[at, 0:SUB], mid[at, SUB : 2 * SUB]))
            for k1, (re, im) in enumerate(fft(items)):
                D[p, k0 + eight * k1, pl.ds(0, SUB, stride=2), :] = re
                D[p, k0 + eight * k1, pl.ds(1, SUB, stride=2), :] = im

    def finish(p):
        for k in col_order:
            col_wait(A.at[p], p, k, p).wait_recv()
        for k in col_order:
            col_part(A.at[p], p, k, p).wait_send()
        z_step(p)

    def opening(p, _):
        y_step(p, A.at[p], p, 0, T)

        @pl.when(p >= 1)
        def _():
            finish(p - 1)

        return 0

    def step(p, _):
        for k in row_order:
            row_wait(p, k, p).wait_recv()
        for k in row_order:
            row_wait(p, k, p).wait_send()
        y_step(p, A.at[p], p, 0, T)
        finish(p - 1)
        return 0

    def localize():
        for k in row_order:
            row_sum_wait(k).wait_recv()
        for k in row_order:
            row_sum(k).wait_send()
        for k in col_order:
            col_sum(k).wait_send()
        total = row_parts[0]
        for r in range(1, R):
            total = total + row_parts[r]
        coef = total * factor
        anomaly = coef - jnp.sum(coef, axis=0, keepdims=True) / plan.members
        columns = 2 * count

        def signed(wave, size):
            return jnp.where(wave < size // 2, wave, wave - size).astype(jnp.float32)

        places = [pick_x.astype(jnp.float32), signed(pick_y, plan.length), signed(pick_z, plan.depth)]
        places = [jnp.concatenate([place, place], axis=1) for place in places]
        squares = places[0] * places[0] + places[1] * places[1] + places[2] * places[2]
        ones = jnp.ones_like(squares)
        nothing = jnp.zeros((LANES - 5, columns), jnp.float32)
        left = jnp.concatenate(places + [squares, ones, nothing], axis=0)
        right = jnp.concatenate([-2.0 * place for place in places] + [ones, squares, nothing], axis=0)
        padded = jnp.concatenate([anomaly, jnp.zeros((LANES - plan.members, columns), jnp.float32)], axis=0)
        left, turned = jnp.transpose(left), jnp.transpose(padded)

        def times(a, b):
            return jnp.dot(a, b, precision=highest, preferred_element_type=jnp.float32)

        for i in range(0, columns, LANES):
            cov = times(turned[i : i + LANES], padded) / (plan.members - 1)
            dist = times(left[i : i + LANES], right)
            localized[i : i + LANES, :] = cov * jnp.exp(-dist / (2.0 * REACH * REACH))

    def whole_first(k):
        return row_copy(
            A.at[pl.ds(0, H), pl.ds((row ^ k) * T, T)], B.at[pl.ds(0, H), pl.ds((row ^ k) * T, T)], 0, k
        )

    for k in row_order:
        whole_first(k).wait_recv()
    for k in row_order:
        whole_first(k).wait_send()
    lax.fori_loop(0, H, opening, 0)
    lax.fori_loop(H, final, step, 0)
    for g in range(groups):
        for k in row_order:
            row_wait(final, k, final + g, g * ply, ply).wait_recv()
        y_step(final, last, final + g, g * ply, ply)
        if g == 0:
            finish(final - 1)
    localize()
    for g in range(groups):
        for k in row_order:
            row_part(final, k, final + g, g * ply, ply).wait_send()
    for g in range(groups):
        for k in col_order:
            col_wait(last, final, k, final + g, g * deep, deep).wait_recv()
            col_part(last, final, k, final + g, g * deep, deep).wait_send()
    z_step(final)


def exchanged(plan, field, modes, factor):
    coarse, fine = waves_of(plan.length, 1.0)
    count = modes.shape[1]
    sums = (plan.members, 2 * count)
    block = (plan.pieces, plan.slabs, 2 * SUB, LANES)
    return pl.pallas_call(
        functools.partial(kernel, plan, factor),
        out_shape=(
            pltpu.VMEM(block, jnp.float32),
            pltpu.VMEM((2 * count, 2 * count), jnp.float32),
        ),
        in_specs=[pl.BlockSpec(memory_space=pl.ANY)] * 4,
        out_specs=(pl.BlockSpec(memory_space=pltpu.VMEM), pl.BlockSpec(memory_space=pltpu.VMEM)),
        scratch_shapes=[
            pltpu.VMEM(block, jnp.float32),
            pltpu.VMEM(block, jnp.float32),
            pltpu.VMEM(block[1:], jnp.float32),
            pltpu.VMEM((2, plan.width, plan.width), jnp.bfloat16),
            pltpu.VMEM((2, plan.length, 2 * plan.length), jnp.bfloat16),
            pltpu.VMEM((2, plan.lanes, 2 * count), jnp.bfloat16),
            pltpu.VMEM((2, plan.lanes, plan.width), jnp.float32),
            pltpu.VMEM((plan.depth, 2 * SUB, LANES), jnp.float32),
            pltpu.VMEM(modes.shape, jnp.int32),
            pltpu.VMEM(coarse.shape, jnp.float32),
            pltpu.VMEM(fine.shape, jnp.float32),
            pltpu.VMEM(sums, jnp.float32),
            pltpu.VMEM(sums, jnp.float32),
            pltpu.VMEM((plan.cols,) + sums, jnp.float32),
            pltpu.VMEM((plan.rows,) + sums, jnp.float32),
            pltpu.SemaphoreType.DMA((plan.pieces + plan.groups,)),
            pltpu.SemaphoreType.DMA((plan.pieces + plan.groups, plan.rows)),
            pltpu.SemaphoreType.DMA((plan.pieces + plan.groups,)),
            pltpu.SemaphoreType.DMA((plan.pieces + plan.groups, plan.cols)),
            pltpu.SemaphoreType.DMA((plan.groups + 2,)),
            pltpu.SemaphoreType.DMA((3,)),
            pltpu.SemaphoreType.DMA((2,)),
            pltpu.SemaphoreType.DMA((plan.cols,)),
            pltpu.SemaphoreType.DMA((plan.rows,)),
        ],
        compiler_params=pltpu.CompilerParams(collective_id=0, has_side_effects=True, vmem_limit_bytes=LIMIT),
    )(field, modes, jnp.asarray(coarse), jnp.asarray(fine))


def settle(plan, piled, square, whole, localized, sems):
    H = plan.parts
    copies = [pltpu.make_async_copy(square, localized, sems.at[plan.pieces])]
    for p in range(plan.pieces):
        m, h = p // H, p % H
        copies.append(pltpu.make_async_copy(piled.at[p], whole.at[:, m, pl.ds(h * 2 * SUB, 2 * SUB), :], sems.at[p]))
    for copy in copies:
        copy.start()
    for copy in copies:
        copy.wait()


def settled(plan, piled, square):
    return pl.pallas_call(
        functools.partial(settle, plan),
        out_shape=(
            jax.ShapeDtypeStruct((plan.depth, plan.members, 2 * plan.waves, plan.local_y), jnp.float32),
            jax.ShapeDtypeStruct(square.shape, jnp.float32),
        ),
        in_specs=[pl.BlockSpec(memory_space=pltpu.VMEM), pl.BlockSpec(memory_space=pltpu.VMEM)],
        out_specs=(pl.BlockSpec(memory_space=pl.ANY), pl.BlockSpec(memory_space=pl.ANY)),
        scratch_shapes=[pltpu.SemaphoreType.DMA((plan.pieces + 1,))],
        compiler_params=pltpu.CompilerParams(vmem_limit_bytes=1 << 20),
    )(pltpu.with_memory_space_constraint(piled, pltpu.VMEM), pltpu.with_memory_space_constraint(square, pltpu.VMEM))


def general(field):
    members = field.shape[2]
    width = field.shape[3]
    rows, cols = lax.axis_size("row"), lax.axis_size("col")
    near, thick = field.shape[0], field.shape[1]
    length, depth = near * rows, thick * cols
    waves = width // 2 // rows
    pieces = PIECES if waves % PIECES == 0 else 1
    part = waves // pieces
    local_y = length // cols
    factor = 1.0 / math.sqrt(NX * NY * NZ)
    cos_x, sin_x = tables(width, width // 2)
    x_table = jnp.stack([cos_x, -sin_x]).reshape(2, width, rows, pieces, part)
    y_table = twiddle(length, length, 1.0).reshape(2, 2, rows, near, length)
    z_table = twiddle(depth, depth, factor).reshape(2, 2, cols, thick, depth)
    flat = field.reshape(near, thick * members, width)
    outs = []
    for piece in range(pieces):
        lines = jnp.einsum("cxrk,ylx->rckyl", x_table[:, :, :, piece], flat, precision=high)
        lines = with_layout_constraint(lines, Layout((0, 1, 2, 3, 4)))
        gathered = lax.all_to_all(lines, "row", split_axis=0, concat_axis=0, tiled=True)
        gathered = with_layout_constraint(gathered, Layout((0, 1, 2, 3, 4)))
        gathered = gathered.reshape(rows, 2, part, near, thick, members)
        ytrans = jnp.einsum("dcsyf,sckyzm->dkmzf", y_table, gathered, precision=high)
        ytrans = ytrans.reshape(2, part, members, thick, cols, local_y)
        ytrans = jnp.transpose(ytrans, (4, 0, 1, 2, 3, 5))
        levels = lax.all_to_all(ytrans, "col", split_axis=0, concat_axis=0, tiled=True)
        outs.append(jnp.einsum("edszg,sdkmzf->gmkef", z_table, levels, precision=high))
    whole = jnp.concatenate(outs, axis=2) if pieces > 1 else outs[0]
    local_q = 2 * waves
    whole = whole.reshape(depth, members, local_q, local_y)
    return whole


def general_localized(whole, modes):
    rows, cols = lax.axis_size("row"), lax.axis_size("col")
    depth, members, local_q, local_y = whole.shape
    waves = local_q // 2
    row_start = lax.axis_index("row") * waves
    col_start = lax.axis_index("col") * local_y
    wave = modes[0] - row_start
    line = modes[1] - col_start
    inside = (wave >= 0) & (wave < waves) & (line >= 0) & (line < local_y)
    wave = jnp.clip(wave, 0, waves - 1)
    line = jnp.clip(line, 0, local_y - 1)
    columns = lax.iota(jnp.int32, local_y)
    tall = whole.reshape(depth, members, waves, 2, local_y)
    picked = tall[modes[2], :, wave]
    hit = (columns[None, :] == line[:, None]) & inside[:, None]
    value = jnp.sum(jnp.where(hit[:, None, None, :], picked, 0.0), axis=-1)
    partial_value = jnp.transpose(value, (1, 2, 0)).reshape(members, -1)
    coef = lax.psum(partial_value, ("row", "col"))
    anomaly = coef - jnp.mean(coef, axis=0, keepdims=True)
    cov = jnp.dot(anomaly.T, anomaly, precision=highest) / (members - 1)
    localized = cov * taper_of(modes, NY, NZ, REACH)
    return localized


def per_device(field, modes):
    plan = Plan(field.shape, lax.axis_size("row"), lax.axis_size("col"))
    factor = 1.0 / math.sqrt(NX * NY * NZ)
    if plan.fits() and modes.shape[1] % LANES == 0:
        whole, localized = settled(plan, *exchanged(plan, field, modes, factor))
    else:
        whole = general(field)
        localized = general_localized(whole, modes)
    return (jnp.transpose(whole, (0, 3, 1, 2)), localized)


def solution(mesh):
    placed = (P("row", "col", None, None), P())
    return jax.shard_map(
        per_device,
        mesh=mesh,
        in_specs=placed,
        out_specs=(P(None, "col", None, "row"), P()),
        check_vma=False,
    )
```

```python
import functools
import math

import jax
import jax.numpy as jnp
import numpy as np
from jax import lax
from jax.experimental import pallas as pl
from jax.experimental.pallas import tpu as pltpu
from jax.experimental.layout import Layout, with_layout_constraint
from jax.sharding import PartitionSpec as P

NX = 512
NY = 512
NZ = 64
REACH = 64


highest = lax.Precision.HIGHEST
high = lax.Precision.HIGH
PIECES = 2


def tables(length, count):
    points = lax.iota(jnp.int32, length)
    waves = lax.iota(jnp.int32, count)
    phase = points[:, None] * waves[None, :] % length
    angle = phase.astype(jnp.float32) * (2.0 * math.pi / length)
    return (jnp.cos(angle), jnp.sin(angle))


def taper_of(modes, size_y, size_z, reach):
    first = modes[0].astype(jnp.float32)
    second = jnp.where(modes[1] < size_y // 2, modes[1], modes[1] - size_y).astype(jnp.float32)
    third = jnp.where(modes[2] < size_z // 2, modes[2], modes[2] - size_z).astype(jnp.float32)
    first = jnp.concatenate([first, first])
    second = jnp.concatenate([second, second])
    third = jnp.concatenate([third, third])
    dist = (first[:, None] - first[None, :]) ** 2 + (second[:, None] - second[None, :]) ** 2
    dist = dist + (third[:, None] - third[None, :]) ** 2
    return jnp.exp(-dist / (2.0 * reach * reach))


def twiddle(length, count, scale):
    cos, sin = tables(length, count)
    cos, sin = cos * scale, sin * scale
    return jnp.stack([jnp.stack([cos, sin]), jnp.stack([-sin, cos])])


MESH = pl.DeviceIdType.MESH
LANES = 128
LIMIT = 49000000
SUB = 8


def split(value):
    top = value.astype(jnp.bfloat16)
    rest = (value - top.astype(jnp.float32)).astype(jnp.bfloat16)
    return top, rest


def waves_of(length, scale):
    j = np.arange(length)
    coarse = 2.0 * np.pi * (np.arange(0, length, SUB)[:, None] * j[None, :] % length) / length
    fine = 2.0 * np.pi * (np.arange(SUB)[:, None] * j[None, :] % length) / length
    coarse = np.stack([np.cos(coarse), np.sin(coarse)]) * scale
    fine = np.stack([np.cos(fine), np.sin(fine)])
    return coarse.astype(np.float32), fine.astype(np.float32)


def cmul(a, c, s):
    re, im = a
    if c == 1.0 and s == 0.0:
        return a
    if c == 0.0 and s == 1.0:
        return im, -re
    return re * c + im * s, im * c - re * s


def fft(items):
    n = len(items)
    if n == 1:
        return items
    even, odd = fft(items[0::2]), fft(items[1::2])
    out = [None] * n
    for k in range(n // 2):
        er, ei = even[k]
        if 8 * k == n or 8 * k == 3 * n:
            r, i = odd[k]
            h = math.sqrt(0.5)
            if 8 * k == n:
                tr, ti = (r + i) * h, (i - r) * h
            else:
                tr, ti = (i - r) * h, (r + i) * (-h)
        elif k == 0:
            tr, ti = odd[k]
        elif 4 * k == n:
            tr, ti = odd[k][1], None
        else:
            angle = 2.0 * math.pi * k / n
            tr, ti = cmul(odd[k], math.cos(angle), math.sin(angle))
        if ti is None:
            r = odd[k][0]
            out[k] = (er + tr, ei - r)
            out[k + n // 2] = (er - tr, ei + r)
        else:
            out[k] = (er + tr, ei + ti)
            out[k + n // 2] = (er - tr, ei - ti)
    return out


class Plan:
    def __init__(self, shape, rows, cols):
        self.near, self.thick, self.members, self.width = shape
        self.rows, self.cols = rows, cols
        self.length = self.near * rows
        self.depth = self.thick * cols
        self.waves = self.width // 2 // rows
        self.local_y = self.length // cols
        self.parts = self.waves // SUB
        self.pieces = self.members * self.parts
        self.lanes = self.near * self.thick
        self.tiles = self.lanes // LANES
        self.slabs = rows * self.tiles
        self.groups = 4

    def fits(self):
        def power(n):
            return n > 1 and n & (n - 1) == 0

        return (
            power(self.rows)
            and power(self.cols)
            and self.waves % SUB == 0
            and self.near * 2 == LANES
            and self.local_y == LANES
            and self.thick % (2 * self.groups) == 0
            and self.members >= 3
            and self.rows % 2 == 0
            and self.slabs == self.cols * self.thick
            and self.depth == 64
            and self.width % 256 == 0
            and self.width == self.length
            and power(self.length)
            and self.members == SUB
        )


EIGHT = 8


def z_transform(source, mid, target):
    for z0 in range(EIGHT):
        items = []
        for z1 in range(EIGHT):
            at = z1 * EIGHT + z0
            items.append((source[at, 0:SUB], source[at, SUB : 2 * SUB]))
        for k0, value in enumerate(fft(items)):
            angle = 2.0 * math.pi * z0 * k0 / 64
            re, im = value if z0 * k0 == 0 else cmul(value, math.cos(angle), math.sin(angle))
            mid[k0 * EIGHT + z0, 0:SUB] = re
            mid[k0 * EIGHT + z0, SUB : 2 * SUB] = im
    for k0 in range(EIGHT):
        items = []
        for z0 in range(EIGHT):
            at = k0 * EIGHT + z0
            items.append((mid[at, 0:SUB], mid[at, SUB : 2 * SUB]))
        for k1, (re, im) in enumerate(fft(items)):
            target[k0 + EIGHT * k1, pl.ds(0, SUB, stride=2), :] = re
            target[k0 + EIGHT * k1, pl.ds(1, SUB, stride=2), :] = im


def kernel(
    plan, factor, field, modes_in, coarse_in, fine_in, D, localized,
    A, B, last, xtab, ytab, ptab, lines, mid, modes, coarse, fine, part, subtotal, col_parts, row_parts,
    row_send, row_recv, col_send, col_recv, in_sem, table_sem, sum_send, sum_col, sum_row,
):
    R, C, H, T = plan.rows, plan.cols, plan.parts, plan.tiles
    near, thick, groups = plan.near, plan.thick, plan.groups
    ply, deep = T // groups, thick // groups
    final = plan.pieces - 1
    row, col = lax.axis_index("row"), lax.axis_index("col")

    def row_peer(k):
        return (row ^ k, col)

    def col_peer(k):
        return (row, col ^ k)

    row_order = list(range(R // 2, R)) + list(range(1, R // 2))
    col_order = list(range(C // 2, C)) + list(range(1, C // 2))

    barrier = pltpu.get_barrier_semaphore()
    for k in range(1, R):
        pl.semaphore_signal(barrier, inc=1, device_id=row_peer(k), device_id_type=MESH)
    for k in range(1, C):
        pl.semaphore_signal(barrier, inc=1, device_id=col_peer(k), device_id_type=MESH)

    def load(m, z, sem):
        at = pl.ds(pl.multiple_of(z * near, near), near)
        return pltpu.make_async_copy(field.at[:, z, m, :], lines.at[m % 2, at, :], in_sem.at[sem])

    tables = [
        pltpu.make_async_copy(coarse_in, coarse, table_sem.at[0]),
        pltpu.make_async_copy(fine_in, fine, table_sem.at[1]),
        pltpu.make_async_copy(modes_in, modes, table_sem.at[2]),
    ]
    for copy in tables:
        copy.start()
    for z in range(thick):
        load(0, z, z // deep).start()

    for copy in tables:
        copy.wait()

    fc, fs = fine[0], fine[1]

    def x_rows(i, _):
        h, r = i // R, i % R
        a = r * H + h
        uc, us = coarse[0, pl.ds(a, 1), :], coarse[1, pl.ds(a, 1), :]
        block = jnp.concatenate([uc * fc - us * fs, -(us * fc + uc * fs)], axis=0)
        top, rest = split(block)
        at = pl.ds(pl.multiple_of(i * 2 * SUB, 2 * SUB), 2 * SUB)
        xtab[0, at, :] = top
        xtab[1, at, :] = rest
        return 0

    lax.fori_loop(0, H * R, x_rows, 0)

    pl.semaphore_wait(barrier, R + C - 2)

    def row_copy(src, dst, unit, k):
        return pltpu.make_async_remote_copy(
            src, dst, row_send.at[unit], row_recv.at[unit, k], device_id=row_peer(k), device_id_type=MESH
        )

    def row_part(p, k, unit, first=0, size=T):
        return row_copy(
            A.at[p, pl.ds((row ^ k) * T + first, size)], B.at[p, pl.ds(row * T + first, size)], unit, k
        )

    def row_wait(p, k, unit, first=0, size=T):
        return row_copy(
            A.at[p, pl.ds((row ^ k) * T + first, size)], B.at[p, pl.ds((row ^ k) * T + first, size)], unit, k
        )

    def col_copy(src, dst, unit, k):
        return pltpu.make_async_remote_copy(
            src, dst, col_send.at[unit], col_recv.at[unit, k], device_id=col_peer(k), device_id_type=MESH
        )

    def col_part(out, p, k, unit, first=0, size=thick):
        return col_copy(
            out.at[pl.ds((col ^ k) * thick + first, size)], D.at[p, pl.ds(col * thick + first, size)], unit, k
        )

    def col_wait(out, p, k, unit, first=0, size=thick):
        return col_copy(
            out.at[pl.ds((col ^ k) * thick + first, size)], D.at[p, pl.ds((col ^ k) * thick + first, size)], unit, k
        )

    def contract(a, b):
        return lax.dot_general(a, b, (((1,), (1,)), ((), ())), preferred_element_type=jnp.float32)

    chunk = ply * LANES

    def x_step(m, g):
        at = pl.ds(pl.multiple_of(g * chunk, chunk), chunk)
        top, rest = split(lines[m % 2, at, :])
        got = contract(xtab[0], top) + (contract(xtab[0], rest) + contract(xtab[1], top))
        for h in range(H):
            for r in range(R):
                base = (h * R + r) * 2 * SUB
                for t in range(ply):
                    A[m * H + h, r * T + g * ply + t] = got[base : base + 2 * SUB, t * LANES : (t + 1) * LANES]

    mine = pl.ds(row * T, T)

    def x_first(g, _):
        for z in range(deep):
            load(0, g * deep + z, g).wait()
        x_step(0, g)
        for k in row_order:
            row_copy(
                A.at[pl.ds(0, H), pl.ds((row ^ k) * T + g * ply, ply)],
                B.at[pl.ds(0, H), pl.ds(row * T + g * ply, ply)],
                0,
                k,
            ).start()
        return 0

    lax.fori_loop(0, groups, x_first, 0)
    for z in range(thick):
        load(1, z, groups + 1).start()
    for h in range(H):
        B[h, mine] = A[h, mine]

    for m in range(1, plan.members):
        if m + 1 < plan.members:
            for z in range(thick):
                load(m + 1, z, groups + (m + 1) % 2).start()
        for z in range(thick):
            load(m, z, groups + m % 2).wait()

        def x_more(g, _):
            x_step(m, g)
            return 0

        lax.fori_loop(0, groups, x_more, 0)
        for h in range(H):
            p = m * H + h
            B[p, mine] = A[p, mine]
            if p < final:
                for k in row_order:
                    row_part(p, k, p).start()
            else:
                for g in range(groups):
                    for k in row_order:
                        row_part(final, k, final + g, g * ply, ply).start()

    count = modes.shape[1]
    pick_x, pick_y, pick_z = modes[0:1, :], modes[1:2, :], modes[2:3, :]

    def phase_rows(t, _):
        cell = t * LANES + lax.broadcasted_iota(jnp.int32, (LANES, count), 0)
        y = row * near + cell % near
        z = col * thick + cell // near
        turns = (pick_y * y + (plan.length // plan.depth) * pick_z * z) % plan.length
        half = (turns - plan.length // 2).astype(jnp.float32) * (math.pi / plan.length)
        square = half * half
        sine, cosine = 1.0, 1.0
        for n in range(6, 0, -1):
            sine = 1.0 - square * sine * (1.0 / (2 * n * (2 * n + 1)))
        for n in range(7, 0, -1):
            cosine = 1.0 - square * cosine * (1.0 / (2 * n * (2 * n - 1)))
        sine = half * sine
        top, rest = split(jnp.concatenate([2.0 * sine * sine - 1.0, -2.0 * sine * cosine], axis=1))
        at = pl.ds(pl.multiple_of(t * LANES, LANES), LANES)
        ptab[0, at, :] = top
        ptab[1, at, :] = rest
        return 0

    lax.fori_loop(0, plan.lanes // LANES, phase_rows, 0)
    part[...] = jnp.zeros_like(part)
    owner = lax.broadcasted_iota(jnp.int32, (R, SUB, count), 0)
    inner = lax.broadcasted_iota(jnp.int32, (R, SUB, count), 1)

    def part_step(p, _):
        m, h = p // H, p % H
        cells = jnp.concatenate(
            [jnp.concatenate([A[p, r * T + t] for t in range(T)], axis=1) for r in range(R)], axis=0
        )
        top, rest = split(cells)

        def times(a, b):
            return jnp.dot(a, b, preferred_element_type=jnp.float32)

        got = times(top, ptab[0]) + (times(rest, ptab[0]) + times(top, ptab[1]))
        got = got.reshape(R, 2, SUB, 2 * count)
        re = got[:, 0, :, :count] + got[:, 1, :, count:]
        im = got[:, 1, :, :count] - got[:, 0, :, count:]
        hit = owner * plan.waves + h * SUB + inner == pick_x.reshape(1, 1, count)
        for c, value in enumerate((re, im)):
            found = jnp.sum(jnp.where(hit, value, 0.0), axis=(0, 1)).reshape(1, count)
            at = slice(c * count, (c + 1) * count)
            part[pl.ds(m, 1), at] = part[pl.ds(m, 1), at] + found
        return 0

    lax.fori_loop(0, plan.pieces, part_step, 0)
    col_parts[col] = part[...]

    def col_sum(k):
        return pltpu.make_async_remote_copy(
            part, col_parts.at[col], sum_send.at[0], sum_col.at[k], device_id=col_peer(k), device_id_type=MESH
        )

    def col_sum_wait(k):
        return pltpu.make_async_remote_copy(
            part, col_parts.at[col ^ k], sum_send.at[0], sum_col.at[k], device_id=col_peer(k), device_id_type=MESH
        )

    def row_sum(k):
        return pltpu.make_async_remote_copy(
            subtotal, row_parts.at[row], sum_send.at[1], sum_row.at[k], device_id=row_peer(k), device_id_type=MESH
        )

    def row_sum_wait(k):
        return pltpu.make_async_remote_copy(
            subtotal, row_parts.at[row ^ k], sum_send.at[1], sum_row.at[k], device_id=row_peer(k), device_id_type=MESH
        )

    for k in col_order:
        col_sum(k).start()

    length = plan.length

    def y_rows(i, _):
        blocks = []
        for b in range(2):
            a = 2 * i + b
            uc, us = coarse[0, pl.ds(a, 1), :], coarse[1, pl.ds(a, 1), :]
            cosine, sine = uc * fc - us * fs, us * fc + uc * fs
            halves = []
            for c in range(C):
                at = slice(c * LANES, (c + 1) * LANES)
                halves += [cosine[:, at], sine[:, at]]
            blocks.append(jnp.concatenate(halves, axis=1))
        top, rest = split(jnp.concatenate(blocks, axis=0) * factor)
        at = pl.ds(pl.multiple_of(i * 2 * SUB, 2 * SUB), 2 * SUB)
        ytab[0, at, :] = top
        ytab[1, at, :] = rest
        return 0

    lax.fori_loop(0, length // (2 * SUB), y_rows, 0)

    for k in col_order:
        col_sum_wait(k).wait_recv()
    total = col_parts[0]
    for c in range(1, C):
        total = total + col_parts[c]
    subtotal[...] = total
    row_parts[row] = total
    for k in row_order:
        row_sum(k).start()


    def y_step(p, out, unit, first, size):
        low = lax.broadcasted_iota(jnp.int32, (size * 2 * SUB, LANES), 1) < near
        evens, odds = [], []
        for t in range(R // 2):
            v0 = B[p, 2 * t * T + first : 2 * t * T + first + size].reshape(size * 2 * SUB, LANES)
            v1 = B[p, (2 * t + 1) * T + first : (2 * t + 1) * T + first + size].reshape(size * 2 * SUB, LANES)
            evens.append(jnp.where(low, v0, pltpu.roll(v1, near, 1)))
            odds.append(jnp.where(low, pltpu.roll(v0, near, 1), v1))
        left = jnp.concatenate([jnp.concatenate(evens, axis=1), jnp.concatenate(odds, axis=1)], axis=0)
        top, rest = split(left)

        def times(a, b):
            return jnp.dot(a, b, preferred_element_type=jnp.float32)

        for k in col_order + [0]:
            c = col ^ k
            at = pl.ds(pl.multiple_of(c * 2 * LANES, 2 * LANES), 2 * LANES)
            both = times(top, ytab[0, :, at]) + (times(rest, ytab[0, :, at]) + times(top, ytab[1, :, at]))
            both = both.reshape(2, size, 2, SUB, 2 * LANES)
            re = both[:, :, 0, :, :LANES] + both[:, :, 1, :, LANES:]
            im = both[:, :, 1, :, :LANES] - both[:, :, 0, :, LANES:]
            for t in range(size):
                for odd in range(2):
                    z = c * thick + 2 * (first + t) + odd
                    if k == 0:
                        D[p, z, 0:SUB] = re[odd, t]
                        D[p, z, SUB : 2 * SUB] = im[odd, t]
                    else:
                        out[z, 0:SUB] = re[odd, t]
                        out[z, SUB : 2 * SUB] = im[odd, t]
            if k != 0:
                col_part(out, p, k, unit, 2 * first, 2 * size).start()

    def finish(p):
        for k in col_order:
            col_wait(A.at[p], p, k, p).wait_recv()
        for k in col_order:
            col_part(A.at[p], p, k, p).wait_send()
        z_transform(D.at[p], mid, D.at[p])

    def opening(p, _):
        y_step(p, A.at[p], p, 0, T)

        @pl.when(p >= 1)
        def _():
            finish(p - 1)

        return 0

    def step(p, _):
        for k in row_order:
            row_wait(p, k, p).wait_recv()
        for k in row_order:
            row_wait(p, k, p).wait_send()
        y_step(p, A.at[p], p, 0, T)
        finish(p - 1)
        return 0

    def localize():
        for k in row_order:
            row_sum_wait(k).wait_recv()
        for k in row_order:
            row_sum(k).wait_send()
        for k in col_order:
            col_sum(k).wait_send()
        total = row_parts[0]
        for r in range(1, R):
            total = total + row_parts[r]
        coef = total * factor
        anomaly = coef - jnp.sum(coef, axis=0, keepdims=True) / plan.members
        columns = 2 * count

        def signed(wave, size):
            return jnp.where(wave < size // 2, wave, wave - size).astype(jnp.float32)

        places = [pick_x.astype(jnp.float32), signed(pick_y, plan.length), signed(pick_z, plan.depth)]
        places = [jnp.concatenate([place, place], axis=1) for place in places]
        squares = places[0] * places[0] + places[1] * places[1] + places[2] * places[2]
        ones = jnp.ones_like(squares)
        nothing = jnp.zeros((LANES - 5, columns), jnp.float32)
        left = jnp.concatenate(places + [squares, ones, nothing], axis=0)
        right = jnp.concatenate([-2.0 * place for place in places] + [ones, squares, nothing], axis=0)
        padded = jnp.concatenate([anomaly, jnp.zeros((LANES - plan.members, columns), jnp.float32)], axis=0)
        left, turned = jnp.transpose(left), jnp.transpose(padded)

        def times(a, b):
            return jnp.dot(a, b, precision=highest, preferred_element_type=jnp.float32)

        for i in range(0, columns, LANES):
            cov = times(turned[i : i + LANES], padded) / (plan.members - 1)
            dist = times(left[i : i + LANES], right)
            localized[i : i + LANES, :] = cov * jnp.exp(-dist / (2.0 * REACH * REACH))

    def whole_first(k):
        return row_copy(
            A.at[pl.ds(0, H), pl.ds((row ^ k) * T, T)], B.at[pl.ds(0, H), pl.ds((row ^ k) * T, T)], 0, k
        )

    for k in row_order:
        whole_first(k).wait_recv()
    for k in row_order:
        whole_first(k).wait_send()
    lax.fori_loop(0, H, opening, 0)
    lax.fori_loop(H, final, step, 0)
    for g in range(groups):
        for k in row_order:
            row_wait(final, k, final + g, g * ply, ply).wait_recv()
        y_step(final, last, final + g, g * ply, ply)
        if g == 0:
            finish(final - 1)
    localize()
    for g in range(groups):
        for k in row_order:
            row_part(final, k, final + g, g * ply, ply).wait_send()
    for g in range(groups):
        for k in col_order:
            col_wait(last, final, k, final + g, g * deep, deep).wait_recv()
            col_part(last, final, k, final + g, g * deep, deep).wait_send()


def exchanged(plan, field, modes, factor):
    coarse, fine = waves_of(plan.length, 1.0)
    count = modes.shape[1]
    sums = (plan.members, 2 * count)
    block = (plan.pieces, plan.slabs, 2 * SUB, LANES)
    return pl.pallas_call(
        functools.partial(kernel, plan, factor),
        out_shape=(
            pltpu.VMEM(block, jnp.float32),
            pltpu.VMEM((2 * count, 2 * count), jnp.float32),
        ),
        in_specs=[pl.BlockSpec(memory_space=pl.ANY)] * 4,
        out_specs=(pl.BlockSpec(memory_space=pltpu.VMEM), pl.BlockSpec(memory_space=pltpu.VMEM)),
        scratch_shapes=[
            pltpu.VMEM(block, jnp.float32),
            pltpu.VMEM(block, jnp.float32),
            pltpu.VMEM(block[1:], jnp.float32),
            pltpu.VMEM((2, plan.width, plan.width), jnp.bfloat16),
            pltpu.VMEM((2, plan.length, 2 * plan.length), jnp.bfloat16),
            pltpu.VMEM((2, plan.lanes, 2 * count), jnp.bfloat16),
            pltpu.VMEM((2, plan.lanes, plan.width), jnp.float32),
            pltpu.VMEM((plan.depth, 2 * SUB, LANES), jnp.float32),
            pltpu.VMEM(modes.shape, jnp.int32),
            pltpu.VMEM(coarse.shape, jnp.float32),
            pltpu.VMEM(fine.shape, jnp.float32),
            pltpu.VMEM(sums, jnp.float32),
            pltpu.VMEM(sums, jnp.float32),
            pltpu.VMEM((plan.cols,) + sums, jnp.float32),
            pltpu.VMEM((plan.rows,) + sums, jnp.float32),
            pltpu.SemaphoreType.DMA((plan.pieces + plan.groups,)),
            pltpu.SemaphoreType.DMA((plan.pieces + plan.groups, plan.rows)),
            pltpu.SemaphoreType.DMA((plan.pieces + plan.groups,)),
            pltpu.SemaphoreType.DMA((plan.pieces + plan.groups, plan.cols)),
            pltpu.SemaphoreType.DMA((plan.groups + 2,)),
            pltpu.SemaphoreType.DMA((3,)),
            pltpu.SemaphoreType.DMA((2,)),
            pltpu.SemaphoreType.DMA((plan.cols,)),
            pltpu.SemaphoreType.DMA((plan.rows,)),
        ],
        compiler_params=pltpu.CompilerParams(collective_id=0, has_side_effects=True, vmem_limit_bytes=LIMIT),
    )(field, modes, jnp.asarray(coarse), jnp.asarray(fine))


def settle(plan, piled, square, whole, localized, mid, stage, sems):
    H = plan.parts
    final = plan.pieces - 1

    def leave(p, source):
        m, h = p // H, p % H
        return pltpu.make_async_copy(source, whole.at[:, m, pl.ds(h * 2 * SUB, 2 * SUB), :], sems.at[p])

    copies = [leave(p, piled.at[p]) for p in range(final)]
    copies.append(pltpu.make_async_copy(square, localized, sems.at[plan.pieces]))
    for copy in copies:
        copy.start()
    z_transform(piled.at[final], mid, stage)
    copies.append(leave(final, stage))
    copies[-1].start()
    for copy in copies:
        copy.wait()


def settled(plan, piled, square):
    return pl.pallas_call(
        functools.partial(settle, plan),
        out_shape=(
            jax.ShapeDtypeStruct((plan.depth, plan.members, 2 * plan.waves, plan.local_y), jnp.float32),
            jax.ShapeDtypeStruct(square.shape, jnp.float32),
        ),
        in_specs=[pl.BlockSpec(memory_space=pltpu.VMEM), pl.BlockSpec(memory_space=pltpu.VMEM)],
        out_specs=(pl.BlockSpec(memory_space=pl.ANY), pl.BlockSpec(memory_space=pl.ANY)),
        scratch_shapes=[
            pltpu.VMEM((plan.depth, 2 * SUB, LANES), jnp.float32),
            pltpu.VMEM((plan.depth, 2 * SUB, LANES), jnp.float32),
            pltpu.SemaphoreType.DMA((plan.pieces + 1,)),
        ],
        compiler_params=pltpu.CompilerParams(vmem_limit_bytes=1 << 22),
    )(pltpu.with_memory_space_constraint(piled, pltpu.VMEM), pltpu.with_memory_space_constraint(square, pltpu.VMEM))


def general(field):
    members = field.shape[2]
    width = field.shape[3]
    rows, cols = lax.axis_size("row"), lax.axis_size("col")
    near, thick = field.shape[0], field.shape[1]
    length, depth = near * rows, thick * cols
    waves = width // 2 // rows
    pieces = PIECES if waves % PIECES == 0 else 1
    part = waves // pieces
    local_y = length // cols
    factor = 1.0 / math.sqrt(NX * NY * NZ)
    cos_x, sin_x = tables(width, width // 2)
    x_table = jnp.stack([cos_x, -sin_x]).reshape(2, width, rows, pieces, part)
    y_table = twiddle(length, length, 1.0).reshape(2, 2, rows, near, length)
    z_table = twiddle(depth, depth, factor).reshape(2, 2, cols, thick, depth)
    flat = field.reshape(near, thick * members, width)
    outs = []
    for piece in range(pieces):
        lines = jnp.einsum("cxrk,ylx->rckyl", x_table[:, :, :, piece], flat, precision=high)
        lines = with_layout_constraint(lines, Layout((0, 1, 2, 3, 4)))
        gathered = lax.all_to_all(lines, "row", split_axis=0, concat_axis=0, tiled=True)
        gathered = with_layout_constraint(gathered, Layout((0, 1, 2, 3, 4)))
        gathered = gathered.reshape(rows, 2, part, near, thick, members)
        ytrans = jnp.einsum("dcsyf,sckyzm->dkmzf", y_table, gathered, precision=high)
        ytrans = ytrans.reshape(2, part, members, thick, cols, local_y)
        ytrans = jnp.transpose(ytrans, (4, 0, 1, 2, 3, 5))
        levels = lax.all_to_all(ytrans, "col", split_axis=0, concat_axis=0, tiled=True)
        outs.append(jnp.einsum("edszg,sdkmzf->gmkef", z_table, levels, precision=high))
    whole = jnp.concatenate(outs, axis=2) if pieces > 1 else outs[0]
    local_q = 2 * waves
    whole = whole.reshape(depth, members, local_q, local_y)
    return whole


def general_localized(whole, modes):
    rows, cols = lax.axis_size("row"), lax.axis_size("col")
    depth, members, local_q, local_y = whole.shape
    waves = local_q // 2
    row_start = lax.axis_index("row") * waves
    col_start = lax.axis_index("col") * local_y
    wave = modes[0] - row_start
    line = modes[1] - col_start
    inside = (wave >= 0) & (wave < waves) & (line >= 0) & (line < local_y)
    wave = jnp.clip(wave, 0, waves - 1)
    line = jnp.clip(line, 0, local_y - 1)
    columns = lax.iota(jnp.int32, local_y)
    tall = whole.reshape(depth, members, waves, 2, local_y)
    picked = tall[modes[2], :, wave]
    hit = (columns[None, :] == line[:, None]) & inside[:, None]
    value = jnp.sum(jnp.where(hit[:, None, None, :], picked, 0.0), axis=-1)
    partial_value = jnp.transpose(value, (1, 2, 0)).reshape(members, -1)
    coef = lax.psum(partial_value, ("row", "col"))
    anomaly = coef - jnp.mean(coef, axis=0, keepdims=True)
    cov = jnp.dot(anomaly.T, anomaly, precision=highest) / (members - 1)
    localized = cov * taper_of(modes, NY, NZ, REACH)
    return localized


def per_device(field, modes):
    plan = Plan(field.shape, lax.axis_size("row"), lax.axis_size("col"))
    factor = 1.0 / math.sqrt(NX * NY * NZ)
    if plan.fits() and modes.shape[1] % LANES == 0:
        whole, localized = settled(plan, *exchanged(plan, field, modes, factor))
    else:
        whole = general(field)
        localized = general_localized(whole, modes)
    return (jnp.transpose(whole, (0, 3, 1, 2)), localized)


def solution(mesh):
    placed = (P("row", "col", None, None), P())
    return jax.shard_map(
        per_device,
        mesh=mesh,
        in_specs=placed,
        out_specs=(P(None, "col", None, "row"), P()),
        check_vma=False,
    )
```
